32 devices in a mesh: shot: 8 (over z, y), rcv: 4 (over x, core).
Axes of the slice: x: 2, y: 2, z: 4, core: 2. Of those that a mesh axis runs over, the one named last changes fastest.
Arguments:
- shot_data: bfloat16 [256, 1024, 256], P('shot', 'rcv'), may hold values from -0.375 to 0.375
- code: int32 [32, 256], P(None, 'shot'), may hold values from -1 to 1, as said below
- observed: bfloat16 [32, 1024, 256], P('shot', 'rcv'), may hold values from -6 to 6
- block_of: int32 [1024, 1], replicated, may hold values from 0 to 3; in each aligned block of 256 rows (0 to 255, 256 to 511, ...) at most 64 rows name the same one
- stencil_index: int32 [1024, 4], replicated, may hold values from 0 to 255
- stencil_weight: float32 [1024, 4], replicated, may hold values from -0.5 to 1
Outputs:
- adjoint_source: float32 [32, 1024, 256], P('shot', 'rcv')
The draws below stay inside these ranges and needn't reach their ends.
Inputs may be any that keep to these rules, and one draw needn't show every extreme that they name: `code`: every entry is -1 or 1. `block_of`: among the receivers of one index of rcv (aligned blocks of 256 rows) at most 64 map to one model block.
All inputs are finite; a program needn't handle non-finite values.
Results may differ from the reference program's by a relative error of at most 0.0038.
Values may be sent and summed in bfloat16 or wider, within the bound.
A program may use at most 64 MiB of HBM per device.

```python
import math
import jax
import jax.numpy as jnp
import numpy as np
from jax import lax

SUPERS = 32
RCV_DEV = 256
SAMPLES = 256
GRID = 256
STENCIL = 4
CAP = 64
SHOTS = 256
RECEIVERS = 1024
BLOCKS = 4


def draw_code(key, part):
    return (2 * jax.random.randint(key, (SUPERS, SHOTS), 0, 2) - 1).astype(jnp.int32)


def plant(array, own_key, least, largest):
    dims = array.shape
    index_at = [jax.random.randint(jax.random.fold_in(own_key, axis), (), 0, dims[axis]) for axis in range(len(dims))]
    array = array.at[tuple(index_at)].set(least)
    longest = dims.index(max(dims))
    index_at[longest] = (index_at[longest] + 1) % dims[longest]
    return array.at[tuple(index_at)].set(largest)


def level_of(rng, shape, shards, smallest, high):
    loudness = 1.0
    for axis_at, shards_of in shards:
        draws = jax.random.uniform(jax.random.fold_in(jax.random.fold_in(rng, 6), axis_at), (shards_of,), jnp.float32, smallest / len(shards), high / len(shards))
        loudness = loudness * jnp.repeat(jnp.exp(draws), shape[axis_at] // shards_of).reshape((-1,) + (1,) * (len(shape) - 1 - axis_at))
    return loudness


def deal_out(rng, own, number, rows, number_of, top, bound, skew):
    order = jax.random.permutation(rng, number_of)
    packed, common = shares(number_of, rows * top, bound, skew, True), shares(number_of, rows * top, bound, skew, False)
    places = jnp.arange(number_of)

    def named(lengths, rotation):
        used = int((lengths > 0).sum())
        fixed = max(1, used // 4)
        shifted = fixed + (places - fixed + rotation * (used - fixed)) % max(1, number_of - fixed)
        return jnp.zeros((number_of,), jnp.int32).at[order[jnp.where(places < fixed, places, shifted)]].set(jnp.asarray(lengths, jnp.int32))

    lengths = jnp.where(number % 4 == 0, named(packed, number // 4), named(common, number - number // 4 - 1))
    mixed = jax.random.permutation(jax.random.fold_in(own, 3), number_of)
    giver, taker = mixed[0:number_of // 2 * 2:2], mixed[1:number_of // 2 * 2:2]
    room = jnp.minimum(lengths[giver] - 1, bound - lengths[taker]) // 2
    room = jnp.where((giver == order[0]) | (taker == order[0]) | (lengths[taker] == 0), 0, jnp.maximum(room, 0))
    shifted = jax.random.randint(jax.random.fold_in(own, 4), (number_of // 2,), 0, 1 << 20) % (room + 1)
    lengths = lengths.at[giver].add(-shifted).at[taker].add(shifted)
    items = jnp.searchsorted(jnp.cumsum(lengths), jnp.arange(rows * top), side="right").astype(jnp.int32)
    listing = items.reshape(top, rows).T
    listing = listing[jax.random.permutation(jax.random.fold_in(own, 1), rows)]
    rotation = jax.random.randint(jax.random.fold_in(own, 2), (rows, 1), 0, top)
    return jnp.take_along_axis(listing, (jnp.arange(top)[None, :] + rotation) % top, axis=1)


def shares(number_of, total, bound, skew, full):
    weights = [(1 << 20) // math.isqrt(rank ** skew) + 1 for rank in range(1, number_of + 1)]
    largest = bound if full else min(bound, max(-(-total // number_of), total * weights[0] // sum(weights)))
    least = 1 if total - largest >= number_of - 1 else 0
    given, spare = [largest] + [least] * (number_of - 1), total - largest - least * (number_of - 1)
    while spare > 0:
        candidates = [i for i in range(1, number_of) if given[i] < largest] or [i for i in range(1, number_of) if given[i] < bound]
        mass, remaining = sum([weights[i] for i in candidates]), spare
        for i in candidates:
            addition = min(bound - given[i], max(1, remaining * weights[i] // mass), spare)
            given[i] = given[i] + addition
            spare = spare - addition
    return np.array(given)


def noise(key, extent, scale, reach, cuts=(), kind=jnp.bfloat16):
    values = jax.random.normal(key, extent, jnp.float32) * scale
    if len(cuts) > 0:
        values = level_of(key, extent, cuts, -0.22, 0.18) * values
    return jnp.clip(values, min=-reach, max=reach).astype(kind)


def setup_inputs(seed: int = 0) -> dict:
    seeds = jax.random.split(jax.random.key(seed), 7)
    shot_data = noise(seeds[0], (SHOTS, RECEIVERS, SAMPLES), SHOTS ** -0.5, 0.375, ((0, 8), (1, 4)))
    code = draw_code(jax.random.fold_in(seeds[6], 71), 0)
    observed = noise(seeds[2], (SUPERS, RECEIVERS, SAMPLES), 1.0, 6.0, ((0, 8), (1, 4)))
    block_of_keys = jax.random.split(jax.random.fold_in(seeds[3], 1), RECEIVERS // RCV_DEV)
    block_of_turns = jax.random.permutation(jax.random.fold_in(seeds[3], 3), RECEIVERS // RCV_DEV)
    block_of = jax.vmap(lambda own, number: deal_out(jax.random.fold_in(seeds[3], 2), own, number, RCV_DEV, BLOCKS, 1, CAP, 2))(block_of_keys, block_of_turns).reshape((RECEIVERS, 1))
    stencil_index = plant(jax.random.randint(seeds[4], (RECEIVERS, STENCIL), 0, GRID), jax.random.fold_in(seeds[4], 1), 0, GRID - 1).astype(jnp.int32)
    stencil_weight = jnp.clip(jax.random.uniform(seeds[5], (RECEIVERS, STENCIL), jnp.float32, -0.5, 1.0), -0.5, 1.0)
    return {"shot_data": shot_data, "code": code, "observed": observed, "block_of": block_of, "stencil_index": stencil_index, "stencil_weight": stencil_weight}


def spread_weights(stencil_index, stencil_weight):
    receivers = stencil_index.shape[0]
    points = jnp.arange(GRID, dtype=jnp.int32)[:, None]
    spread = jnp.zeros((GRID, receivers), jnp.float32)
    for which in range(STENCIL):
        spread = spread + jnp.where(points == stencil_index[:, which][None, :], stencil_weight[:, which][None, :], 0.0)
    return spread


def reference(shot_data, code, observed, block_of, stencil_index, stencil_weight):
    shots, receivers, samples = shot_data.shape
    flat_rows = shot_data.reshape(shots, receivers * samples)
    supershot = jnp.dot(code.astype(jnp.bfloat16), flat_rows, preferred_element_type=jnp.float32)
    supershot = supershot.reshape(SUPERS, receivers, samples)
    residual = (supershot - observed.astype(jnp.float32)).astype(jnp.bfloat16)
    spread = spread_weights(stencil_index, stencil_weight)
    block_ids = jnp.arange(BLOCKS, dtype=jnp.int32)[:, None, None]
    injection = jnp.where(block_ids == block_of[:, 0][None, None, :], spread[None], 0.0)
    injection = injection.reshape(BLOCKS * GRID, receivers).astype(jnp.bfloat16)
    return jnp.einsum("cr,krt->kct", injection.astype(jnp.float32), residual.astype(jnp.float32), precision=lax.Precision.HIGHEST)
```

```python
import functools

import jax
import jax.numpy as jnp
from jax import lax
from jax.experimental import pallas as pl
from jax.experimental.pallas import tpu as pltpu
from jax.sharding import PartitionSpec as P

GRID = 256
CAP = 64
ROWS = 16
LANES = 128
CUTS = 2
AHEAD = 2
LAG = 2.5
LOW_FIRST = (1, 4, 7, 10)
DIRECT = 2

BF16, F32 = jnp.bfloat16, jnp.float32
MESH = pl.DeviceIdType.MESH


def stages_of(piece, pieces, bits):
    rest = [(bit,) for bit in range(2, bits)]
    if bits == 1:
        return [(0,)]
    if piece >= pieces - DIRECT:
        return [(0,), tuple(range(1, bits))]
    if piece in LOW_FIRST:
        return [(1,), (0,)] + rest
    return [(0,), (1,)] + rest


def plan(pieces, bits):
    table, sems = [], 0
    for piece in range(pieces):
        left, slot, stages = list(range(1 << bits)), 0, []
        for group in stages_of(piece, pieces, bits):
            mask = sum(1 << bit for bit in group)
            kept = [m for m in left if not m & mask]
            peers = []
            for peer in range(1, 1 << bits):
                if peer & ~mask:
                    continue
                peers.append((peer, slot, sems))
                slot, sems = slot + len(kept), sems + 1
            stages.append((kept, peers))
            left = kept
        table.append(stages)
    return table, sems


def schedule(table, halves_of):
    tasks = []
    for p, stages in enumerate(table):
        tasks.append((max(p - AHEAD, -1), 0, p, "encode", 0))
        for s in range(len(stages) - 1):
            tasks.append((p + LAG * s, 1, p, "sum", s))
    for c, members in enumerate(halves_of):
        done = max(p + LAG * (len(table[p]) - 1) for p in members)
        tasks.append((done, 2, c, "finish", 0))
        tasks.append((done + LAG, 3, c, "inject", 0))
    return sorted(tasks)


def kernel(dims, table, shot_hbm, code_hbm, obs_hbm, blk_hbm, idx_hbm, wgt_hbm, out,
           shot, code_ref, obs, blk_ref, idx_ref, wgt_ref, signs, weights, acc, send, recv,
           send3, recv3, select, slotm, load_sem, ssem, rsem, s3, r3):
    n, groups, owned, halves = dims
    bits = n.bit_length() - 1
    shots, rcv, _ = shot_hbm.shape
    part = rcv // CUTS
    chunks = owned * halves
    slots = groups * CAP
    me = lax.axis_index("shot")
    mine = lax.axis_index("rcv")

    def partner(mask):
        at = me
        for bit in range(bits):
            if mask >> bit & 1:
                own = lax.rem(lax.div(me, 1 << bit), 2)
                at = at + (1 << bit) - own * (2 << bit)
        return at

    partners = [partner(mask) for mask in range(n)]

    def rcv_peer(e):
        return lax.rem(mine + e, groups)

    def cut(h):
        return pl.ds(h * LANES, LANES)

    small = [(code_hbm, code_ref), (blk_hbm, blk_ref), (idx_hbm, idx_ref), (wgt_hbm, wgt_ref),
             (obs_hbm, obs)]
    small = [pltpu.make_async_copy(src, dst, load_sem.at[i]) for i, (src, dst) in enumerate(small)]
    loads = {}
    for h in range(halves):
        for q in range(CUTS):
            some = pl.ds(q * part, part)
            loads[h, q] = pltpu.make_async_copy(
                shot_hbm.at[:, some, cut(h)], shot.at[h, :, some, :],
                load_sem.at[len(small) + h * CUTS + q])
    small[0].start()
    for load in loads.values():
        load.start()
    for load in small[1:]:
        load.start()

    barrier = pltpu.get_barrier_semaphore()
    for mask in range(1, n):
        pl.semaphore_signal(barrier, inc=1, device_id={"shot": partners[mask]}, device_id_type=MESH)
    for e in range(1, groups):
        pl.semaphore_signal(barrier, inc=1, device_id={"rcv": rcv_peer(e)}, device_id_type=MESH)

    out_rows, depth = n * ROWS, shots * ROWS
    spread_s = (lax.broadcasted_iota(jnp.int32, (shots, depth), 1)
                - ROWS * lax.broadcasted_iota(jnp.int32, (shots, depth), 0))
    spread_s = ((spread_s >= 0) & (spread_s < ROWS)).astype(F32).astype(BF16)

    def widen(j):
        same_row = ((lax.broadcasted_iota(jnp.int32, (out_rows, depth), 0) & (ROWS - 1))
                    == (lax.broadcasted_iota(jnp.int32, (out_rows, depth), 1) & (ROWS - 1)))
        for m in range(n):
            line = code_ref[pl.ds(partners[m] * owned + j, 1), :].astype(F32)
            signs[j, m * ROWS:(m + 1) * ROWS, :] = jnp.broadcast_to(line, (ROWS, shots)).astype(BF16)
        wide = jnp.dot(signs[j], spread_s, preferred_element_type=F32)
        weights[j] = jnp.where(same_row, wide, 0.0).astype(BF16)

    def copies(p, s):
        kept, peers = table[p][s]
        return [pltpu.make_async_remote_copy(
            src_ref=send.at[p, pl.ds(slot, len(kept))], dst_ref=recv.at[p, pl.ds(slot, len(kept))],
            send_sem=ssem.at[sem], recv_sem=rsem.at[sem],
            device_id={"shot": partners[peer]}, device_id_type=MESH)
            for peer, slot, sem in peers]

    def copy3(c, e):
        return pltpu.make_async_remote_copy(
            src_ref=send3.at[c, e - 1], dst_ref=recv3.at[c, e], send_sem=s3.at[c, e - 1],
            recv_sem=r3.at[c, e - 1], device_id={"rcv": rcv_peer(e)}, device_id_type=MESH)

    def place(p):
        return p // (halves * CUTS), p // CUTS % halves, p % CUTS

    def encode(p, _):
        j, h, q = place(p)
        if h == 0 and q == 0:
            if j == 0:
                small[0].wait()
            widen(j)
        if j == 0:
            loads[h, q].wait()
        kept, peers = table[p][0]

        def tile(g, carry):
            rows = pl.ds(pl.multiple_of(g * ROWS, ROWS), ROWS)
            x = shot[h, :, pl.ds(pl.multiple_of(q * part + g * ROWS, ROWS), ROWS), :]
            y = jnp.dot(weights[j], x.reshape(depth, LANES), preferred_element_type=F32)
            y = y.reshape(n, ROWS, LANES)
            for m in kept:
                acc[p, m, rows, :] = y[m]
            for peer, slot, _ in peers:
                for i, m in enumerate(kept):
                    send[p, slot + i, rows, :] = y[m | peer].astype(BF16)
            return carry

        lax.fori_loop(0, part // ROWS, tile, 0, unroll=4)
        if p == 0:
            pl.semaphore_wait(barrier, n + groups - 2)
        for copy in copies(p, 0):
            copy.start()

    def received(p, s, m):
        kept, peers = table[p][s]
        total = acc[p, m]
        for _, slot, _ in peers:
            total = total + recv[p, slot + kept.index(m)].astype(F32)
        return total

    def sum_up(p, s):
        for copy in copies(p, s):
            copy.wait_recv()
        kept, peers = table[p][s + 1]
        for (peer, slot, _), copy in zip(peers, copies(p, s + 1)):
            for i, m in enumerate(kept):
                send[p, slot + i] = received(p, s, m | peer).astype(BF16)
            copy.start()
        for m in kept:
            acc[p, m] = received(p, s, m)

    def finish(c, _):
        j, h = c // halves, c % halves
        picked = jnp.zeros((slots, LANES), F32)
        for q in range(CUTS):
            p = c * CUTS + q
            for copy in copies(p, len(table[p]) - 1):
                copy.wait_recv()
            some = pl.ds(q * part, part)
            residual = received(p, len(table[p]) - 1, 0) - obs[j, some, cut(h)].astype(F32)
            picked = picked + jnp.dot(
                select[:, some], residual.astype(BF16), preferred_element_type=F32)
        picked = picked.astype(BF16)
        for e in range(1, groups):
            send3[c, e - 1] = picked[e * CAP:(e + 1) * CAP]
            copy3(c, e).start()
        recv3[c, 0] = picked[:CAP]

    def inject(c, _):
        for e in range(1, groups):
            copy3(c, e).wait_recv()
        arrived = recv3[c].reshape(slots, LANES)
        j, h = c // halves, c % halves
        out[j, :, cut(h)] = jnp.dot(slotm[...], arrived, preferred_element_type=F32)

    def prepare():
        before = (lax.broadcasted_iota(jnp.int32, (rcv, rcv), 0)
                  < lax.broadcasted_iota(jnp.int32, (rcv, rcv), 1)).astype(F32).astype(BF16)
        slot_at = lax.broadcasted_iota(jnp.int32, (slots, rcv), 0)
        point_at = lax.broadcasted_iota(jnp.int32, (GRID, rcv), 0)
        block_at = lax.broadcasted_iota(jnp.int32, (max(16, groups), rcv), 0)

        def rank_of(ids):
            hot = (block_at == ids).astype(F32)
            count = jnp.dot(hot.astype(BF16), before, preferred_element_type=F32)
            return jnp.sum(hot * count, axis=0, keepdims=True).astype(jnp.int32)

        total = jnp.zeros((GRID, slots), F32)
        for e in range(groups):
            source = lax.rem(mine - e + groups, groups)
            at = pl.ds(pl.multiple_of(source * rcv, rcv), rcv)
            ids = blk_ref[:, at]
            rank = rank_of(ids)
            if e == 0:
                ahead = ids - mine
                ahead = jnp.where(ahead < 0, ahead + groups, ahead)
                select[...] = (slot_at == ahead * CAP + rank).astype(F32).astype(BF16)
            spread = jnp.zeros((GRID, rcv), F32)
            for w in range(idx_ref.shape[0]):
                spread = spread + jnp.where(
                    point_at == idx_ref[pl.ds(w, 1), at], wgt_ref[pl.ds(w, 1), at], 0.0)
            key = jnp.where(ids == mine, e * CAP + rank, -1)
            pick = (slot_at == key).astype(F32).astype(BF16)
            total = total + lax.dot_general(
                spread.astype(BF16), pick, (((1,), (1,)), ((), ())), preferred_element_type=F32)
        slotm[...] = total.astype(BF16)

    act = {"encode": encode, "sum": sum_up, "finish": finish, "inject": inject}
    prepared = False
    members = [[c * CUTS + q for q in range(CUTS)] for c in range(chunks)]
    for _, _, item, what, s in schedule(table, members):
        if what != "encode" and not prepared:
            for load in small[1:]:
                load.wait()
            prepare()
            prepared = True
        act[what](item, s)
    for p in range(len(table)):
        for s in range(len(table[p])):
            for copy in copies(p, s):
                copy.wait_send()
    for c in range(chunks):
        for e in range(1, groups):
            copy3(c, e).wait_send()


def on_device(n_shot, n_rcv, shot_data, code, observed, block_of, stencil_index, stencil_weight):
    shots, rcv, samples = shot_data.shape
    owned = observed.shape[0]
    halves = samples // LANES
    chunks = owned * halves
    pieces = chunks * CUTS
    part = rcv // CUTS
    slots = n_rcv * CAP
    table, sems = plan(pieces, n_shot.bit_length() - 1)
    hbm = pl.BlockSpec(memory_space=pltpu.HBM)
    vmem = pltpu.VMEM
    dma = pltpu.SemaphoreType.DMA
    rows = (block_of.T, stencil_index.T, stencil_weight.T)
    return pl.pallas_call(
        functools.partial(kernel, (n_shot, n_rcv, owned, halves), table),
        out_shape=pltpu.VMEM((owned, GRID, samples), F32),
        in_specs=[hbm] * 6,
        out_specs=pl.BlockSpec(memory_space=vmem),
        scratch_shapes=[
            vmem((halves, shots, rcv, LANES), BF16),
            vmem(code.shape, code.dtype),
            vmem((owned, rcv, samples), BF16),
            *[vmem(row.shape, row.dtype) for row in rows],
            vmem((owned, n_shot * ROWS, shots), BF16),
            vmem((owned, n_shot * ROWS, shots * ROWS), BF16),
            vmem((pieces, n_shot, part, LANES), F32),
            vmem((pieces, n_shot - 1, part, LANES), BF16),
            vmem((pieces, n_shot - 1, part, LANES), BF16),
            vmem((chunks, n_rcv - 1, CAP, LANES), BF16),
            vmem((chunks, n_rcv, CAP, LANES), BF16),
            vmem((slots, rcv), BF16),
            vmem((GRID, slots), BF16),
            dma((5 + halves * CUTS,)),
            dma((sems,)),
            dma((sems,)),
            dma((chunks, n_rcv - 1)),
            dma((chunks, n_rcv - 1)),
        ],
        compiler_params=pltpu.CompilerParams(
            collective_id=0, has_side_effects=True, vmem_limit_bytes=40 * 2**20),
    )(*[pltpu.with_memory_space_constraint(x, pltpu.HBM)
        for x in (shot_data, code, observed, *rows)])


def solution(mesh):
    placed = (P("shot", "rcv", None), P(None, "shot"), P("shot", "rcv", None), P(), P(), P())
    body = functools.partial(on_device, mesh.shape["shot"], mesh.shape["rcv"])
    return jax.shard_map(
        body, mesh=mesh, in_specs=placed, out_specs=P("shot", "rcv", None), check_vma=False
    )
```

```python
import functools

import jax
import jax.numpy as jnp
from jax import lax
from jax.experimental import pallas as pl
from jax.experimental.pallas import tpu as pltpu
from jax.sharding import PartitionSpec as P

GRID = 256
CAP = 64
ROWS = 16
LANES = 128
CUTS = 4
AHEAD = 4
LAG = 4
HOLD = 3
DIRECT = 5
LOW_FIRST = 5 / 32
LOW_SPAN = 20 / 32

BF16, F32 = jnp.bfloat16, jnp.float32
MESH = pl.DeviceIdType.MESH


def stages_of(piece, pieces, bits):
    rest = [(bit,) for bit in range(1, bits)]
    low = max(1, round(pieces * LOW_FIRST))
    span = round(pieces * LOW_SPAN)
    if bits == 1:
        return [(0,)]
    if piece >= pieces - DIRECT:
        return [(0,), tuple(range(1, bits))]
    if piece in [1 + i * (span - 1) // low for i in range(low)]:
        return rest + [(0,)]
    return [(0,)] + rest


def plan(pieces, bits):
    table, sems = [], 0
    for piece in range(pieces):
        left, slot, stages = list(range(1 << bits)), 0, []
        for group in stages_of(piece, pieces, bits):
            mask = sum(1 << bit for bit in group)
            kept = [m for m in left if not m & mask]
            first, peers = slot, []
            for peer in range(1, 1 << bits):
                if not peer & ~mask:
                    peers.append((peer, slot))
                    slot += len(kept)
            stages.append((kept, peers, (first, slot - first), sems))
            left, sems = kept, sems + 1
        table.append(stages)
    return table, sems


def schedule(table, halves_of):
    hold, tasks, done = len(table) - HOLD, [], []
    for p, stages in enumerate(table):
        late = stages[0][1][0][0] != 1
        tasks.append((max(p - AHEAD, -1), 0, p, "encode", 0))
        for s in range(len(stages) - 1):
            at = p + LAG * s
            if late and s == len(stages) - 2:
                at = max(at, hold)
            tasks.append((at, 1, p, "sum", s))
        at = p + LAG * (len(stages) - 1)
        done.append(max(at, hold + LAG) if late else at)
    for c, members in enumerate(halves_of):
        at = max(done[p] for p in members)
        tasks.append((at, 2, c, "finish", 0))
        tasks.append((at + LAG, 3, c, "inject", 0))
    return sorted(tasks)


def kernel(dims, table, shot_hbm, code_hbm, obs_hbm, blk_hbm, idx_hbm, wgt_hbm, out,
           shot, code_ref, obs, blk_ref, idx_ref, wgt_ref, signs, weights, acc, send, recv,
           send3, recv3, select, slotm, load_sem, ssem, rsem, s3, r3):
    n, groups, owned, halves = dims
    bits = n.bit_length() - 1
    shots, rcv, _ = shot_hbm.shape
    part = rcv // CUTS
    chunks = owned * halves
    slots = groups * CAP
    me = lax.axis_index("shot")
    mine = lax.axis_index("rcv")

    def partner(mask):
        at = me
        for bit in range(bits):
            if mask >> bit & 1:
                own = lax.rem(lax.div(me, 1 << bit), 2)
                at = at + (1 << bit) - own * (2 << bit)
        return at

    partners = [partner(mask) for mask in range(n)]

    def rcv_peer(e):
        return lax.rem(mine + e, groups)

    def cut(h):
        return pl.ds(h * LANES, LANES)

    small = [(code_hbm, code_ref), (blk_hbm, blk_ref), (idx_hbm, idx_ref), (wgt_hbm, wgt_ref),
             (obs_hbm, obs)]
    small = [pltpu.make_async_copy(src, dst, load_sem.at[i]) for i, (src, dst) in enumerate(small)]
    loads = {}
    for h in range(halves):
        for q in range(CUTS):
            some = pl.ds(q * part, part)
            loads[h, q] = pltpu.make_async_copy(
                shot_hbm.at[:, some, cut(h)], shot.at[h, :, some, :],
                load_sem.at[len(small) + h * CUTS + q])
    small[0].start()
    for load in loads.values():
        load.start()
    for load in small[1:]:
        load.start()

    barrier = pltpu.get_barrier_semaphore()
    near = [1 << bit for bit in range(bits)]
    for mask in near:
        pl.semaphore_signal(barrier, inc=1, device_id={"shot": partners[mask]}, device_id_type=MESH)
    for e in range(1, groups):
        pl.semaphore_signal(barrier, inc=1, device_id={"rcv": rcv_peer(e)}, device_id_type=MESH)

    out_rows, depth = n * ROWS, shots * ROWS
    spread_s = (lax.broadcasted_iota(jnp.int32, (shots, depth), 1)
                - ROWS * lax.broadcasted_iota(jnp.int32, (shots, depth), 0))
    spread_s = ((spread_s >= 0) & (spread_s < ROWS)).astype(F32).astype(BF16)

    def widen(j):
        same_row = ((lax.broadcasted_iota(jnp.int32, (out_rows, depth), 0) & (ROWS - 1))
                    == (lax.broadcasted_iota(jnp.int32, (out_rows, depth), 1) & (ROWS - 1)))
        for m in range(n):
            line = code_ref[pl.ds(partners[m] * owned + j, 1), :].astype(F32)
            signs[j, m * ROWS:(m + 1) * ROWS, :] = jnp.broadcast_to(line, (ROWS, shots)).astype(BF16)
        wide = jnp.dot(signs[j], spread_s, preferred_element_type=F32)
        weights[j] = jnp.where(same_row, wide, 0.0).astype(BF16)

    def copy_of(p, slot, count, sem, peer):
        c, some = p // CUTS, pl.ds(p % CUTS * part, part)
        return pltpu.make_async_remote_copy(
            src_ref=send.at[c, pl.ds(slot, count), some], dst_ref=recv.at[c, pl.ds(slot, count), some],
            send_sem=ssem, recv_sem=rsem.at[sem],
            device_id={"shot": partners[peer]}, device_id_type=MESH)

    def copies(p, s):
        kept, peers, _, sem = table[p][s]
        return [copy_of(p, slot, len(kept), sem, peer) for peer, slot in peers]

    def wait_for(p, s):
        _, peers, (first, count), sem = table[p][s]
        copy_of(p, first, count, sem, peers[0][0]).wait_recv()

    def copy3(c, e):
        return pltpu.make_async_remote_copy(
            src_ref=send3.at[c, e - 1], dst_ref=recv3.at[c, e], send_sem=s3,
            recv_sem=r3.at[c], device_id={"rcv": rcv_peer(e)}, device_id_type=MESH)

    def copies3(c):
        return pltpu.make_async_remote_copy(
            src_ref=send3.at[c], dst_ref=recv3.at[c, pl.ds(1, groups - 1)], send_sem=s3,
            recv_sem=r3.at[c], device_id={"rcv": rcv_peer(1)}, device_id_type=MESH)

    def place(p):
        return p // (halves * CUTS), p // CUTS % halves, p % CUTS

    def encode(p, _):
        j, h, q = place(p)
        if h == 0 and q == 0:
            if j == 0:
                small[0].wait()
            widen(j)
        if j == 0:
            loads[h, q].wait()
        kept, peers, _, _ = table[p][0]
        c = p // CUTS

        def tile(g, carry):
            rows = pl.ds(pl.multiple_of(q * part + g * ROWS, ROWS), ROWS)
            x = shot[h, :, rows, :]
            y = jnp.dot(weights[j], x.reshape(depth, LANES), preferred_element_type=F32)
            y = y.reshape(n, ROWS, LANES)
            for m in kept:
                acc[c, m, rows, :] = y[m]
            for peer, slot in peers:
                for i, m in enumerate(kept):
                    send[c, slot + i, rows, :] = y[m | peer].astype(BF16)
            return carry

        lax.fori_loop(0, part // ROWS, tile, 0, unroll=4)
        if p == 0:
            pl.semaphore_wait(barrier, len(near) + groups - 1)
        for copy in copies(p, 0):
            copy.start()

    def received(p, s, m):
        kept, peers, _, _ = table[p][s]
        c, some = p // CUTS, pl.ds(p % CUTS * part, part)
        total = acc[c, m, some]
        for _, slot in peers:
            total = total + recv[c, slot + kept.index(m), some].astype(F32)
        return total

    def sum_up(p, s):
        wait_for(p, s)
        kept, peers, _, _ = table[p][s + 1]
        c, some = p // CUTS, pl.ds(p % CUTS * part, part)
        for (peer, slot), copy in zip(peers, copies(p, s + 1)):
            for i, m in enumerate(kept):
                send[c, slot + i, some] = received(p, s, m | peer).astype(BF16)
            copy.start()
        for m in kept:
            acc[c, m, some] = received(p, s, m)

    def finish(c, _):
        j, h = c // halves, c % halves
        picked = jnp.zeros((slots, LANES), F32)
        for q in range(CUTS):
            p = c * CUTS + q
            wait_for(p, len(table[p]) - 1)
            some = pl.ds(q * part, part)
            residual = received(p, len(table[p]) - 1, 0) - obs[j, some, cut(h)].astype(F32)
            picked = picked + jnp.dot(
                select[:, some], residual.astype(BF16), preferred_element_type=F32)
        picked = picked.astype(BF16)
        for e in range(1, groups):
            send3[c, e - 1] = picked[e * CAP:(e + 1) * CAP]
            copy3(c, e).start()
        recv3[c, 0] = picked[:CAP]

    def inject(c, _):
        copies3(c).wait_recv()
        arrived = recv3[c].reshape(slots, LANES)
        j, h = c // halves, c % halves
        out[j, :, cut(h)] = jnp.dot(slotm[...], arrived, preferred_element_type=F32)

    def prepare():
        before = (lax.broadcasted_iota(jnp.int32, (rcv, rcv), 0)
                  < lax.broadcasted_iota(jnp.int32, (rcv, rcv), 1)).astype(F32).astype(BF16)
        slot_at = lax.broadcasted_iota(jnp.int32, (slots, rcv), 0)
        point_at = lax.broadcasted_iota(jnp.int32, (GRID, rcv), 0)
        block_at = lax.broadcasted_iota(jnp.int32, (max(16, groups), rcv), 0)

        def rank_of(ids):
            hot = (block_at == ids).astype(F32)
            count = jnp.dot(hot.astype(BF16), before, preferred_element_type=F32)
            return jnp.sum(hot * count, axis=0, keepdims=True).astype(jnp.int32)

        total = jnp.zeros((GRID, slots), F32)
        for e in range(groups):
            source = lax.rem(mine - e + groups, groups)
            at = pl.ds(pl.multiple_of(source * rcv, rcv), rcv)
            ids = blk_ref[:, at]
            rank = rank_of(ids)
            if e == 0:
                ahead = ids - mine
                ahead = jnp.where(ahead < 0, ahead + groups, ahead)
                select[...] = (slot_at == ahead * CAP + rank).astype(F32).astype(BF16)
            spread = jnp.zeros((GRID, rcv), F32)
            for w in range(idx_ref.shape[0]):
                spread = spread + jnp.where(
                    point_at == idx_ref[pl.ds(w, 1), at], wgt_ref[pl.ds(w, 1), at], 0.0)
            key = jnp.where(ids == mine, e * CAP + rank, -1)
            pick = (slot_at == key).astype(F32).astype(BF16)
            total = total + lax.dot_general(
                spread.astype(BF16), pick, (((1,), (1,)), ((), ())), preferred_element_type=F32)
        slotm[...] = total.astype(BF16)

    act = {"encode": encode, "sum": sum_up, "finish": finish, "inject": inject}
    prepared = False
    members = [[c * CUTS + q for q in range(CUTS)] for c in range(chunks)]
    for _, _, item, what, s in schedule(table, members):
        if what != "encode" and not prepared:
            for load in small[1:]:
                load.wait()
            prepare()
            prepared = True
        act[what](item, s)
    pltpu.make_async_remote_copy(
        src_ref=send, dst_ref=recv, send_sem=ssem, recv_sem=rsem.at[0],
        device_id={"shot": partners[1]}, device_id_type=MESH).wait_send()
    pltpu.make_async_remote_copy(
        src_ref=send3, dst_ref=send3, send_sem=s3, recv_sem=r3.at[0],
        device_id={"rcv": rcv_peer(1)}, device_id_type=MESH).wait_send()


def on_device(n_shot, n_rcv, shot_data, code, observed, block_of, stencil_index, stencil_weight):
    shots, rcv, samples = shot_data.shape
    owned = observed.shape[0]
    halves = samples // LANES
    chunks = owned * halves
    pieces = chunks * CUTS
    slots = n_rcv * CAP
    table, sems = plan(pieces, n_shot.bit_length() - 1)
    hbm = pl.BlockSpec(memory_space=pltpu.HBM)
    vmem = pltpu.VMEM
    dma = pltpu.SemaphoreType.DMA
    rows = (block_of.T, stencil_index.T, stencil_weight.T)
    return pl.pallas_call(
        functools.partial(kernel, (n_shot, n_rcv, owned, halves), table),
        out_shape=pltpu.VMEM((owned, GRID, samples), F32),
        in_specs=[hbm] * 6,
        out_specs=pl.BlockSpec(memory_space=vmem),
        scratch_shapes=[
            vmem((halves, shots, rcv, LANES), BF16),
            vmem(code.shape, code.dtype),
            vmem((owned, rcv, samples), BF16),
            *[vmem(row.shape, row.dtype) for row in rows],
            vmem((owned, n_shot * ROWS, shots), BF16),
            vmem((owned, n_shot * ROWS, shots * ROWS), BF16),
            vmem((chunks, n_shot, rcv, LANES), F32),
            vmem((chunks, n_shot - 1, rcv, LANES), BF16),
            vmem((chunks, n_shot - 1, rcv, LANES), BF16),
            vmem((chunks, n_rcv - 1, CAP, LANES), BF16),
            vmem((chunks, n_rcv, CAP, LANES), BF16),
            vmem((slots, rcv), BF16),
            vmem((GRID, slots), BF16),
            dma((5 + halves * CUTS,)),
            dma,
            dma((sems,)),
            dma,
            dma((chunks,)),
        ],
        compiler_params=pltpu.CompilerParams(
            collective_id=0, has_side_effects=True, vmem_limit_bytes=40 * 2**20),
    )(*[pltpu.with_memory_space_constraint(x, pltpu.HBM)
        for x in (shot_data, code, observed, *rows)])


def solution(mesh):
    placed = (P("shot", "rcv", None), P(None, "shot"), P("shot", "rcv", None), P(), P(), P())
    body = functools.partial(on_device, mesh.shape["shot"], mesh.shape["rcv"])
    return jax.shard_map(
        body, mesh=mesh, in_specs=placed, out_specs=P("shot", "rcv", None), check_vma=False
    )
```

```python
import functools

import jax
import jax.numpy as jnp
from jax import lax
from jax.experimental import pallas as pl
from jax.experimental.pallas import tpu as pltpu
from jax.sharding import PartitionSpec as P

GRID = 256
CAP = 64
ROWS = 16
LANES = 128
CUTS = 4
AHEAD = 4
LAG = 4
HOLD = 3
DIRECT = 5
SPLIT = 0
LOW_FIRST = 5 / 32
LOW_SPAN = 20 / 32

BF16, F32 = jnp.bfloat16, jnp.float32
MESH = pl.DeviceIdType.MESH


def stages_of(piece, pieces, bits):
    rest = [(bit,) for bit in range(1, bits)]
    low = max(1, round(pieces * LOW_FIRST))
    span = round(pieces * LOW_SPAN)
    if bits == 1:
        return [(0,)]
    if piece >= pieces - DIRECT:
        return [(0,), tuple(range(1, bits))]
    if piece in [1 + i * (span - 1) // low for i in range(low)]:
        return rest + [(0,)]
    return [(0,)] + rest


def cut_up(chunks, rcv):
    part = rcv // CUTS
    pieces = [(c, q * part, part) for c in range(chunks) for q in range(CUTS)]
    for _ in range(SPLIT if part % (2 * ROWS) == 0 else 0):
        c, row, rows = pieces.pop()
        pieces += [(c, row, rows // 2), (c, row + rows // 2, rows // 2)]
    return pieces


def plan(pieces, bits):
    table = []
    for piece in range(pieces):
        left, slot, stages = list(range(1 << bits)), 0, []
        for group in stages_of(piece, pieces, bits):
            mask = sum(1 << bit for bit in group)
            kept = [m for m in left if not m & mask]
            first, peers = slot, []
            for peer in range(1, 1 << bits):
                if not peer & ~mask:
                    peers.append((peer, slot))
                    slot += len(kept)
            stages.append((kept, peers, (first, slot - first)))
            left = kept
        table.append(stages)
    return table


def schedule(table, halves_of):
    hold, tasks, done = len(table) - HOLD, [], []
    for p, stages in enumerate(table):
        late = stages[0][1][0][0] != 1
        tasks.append((max(p - AHEAD, -1), 0, p, "encode", 0))
        for s in range(len(stages) - 1):
            at = p + LAG * s
            if late and s == len(stages) - 2:
                at = max(at, hold)
            tasks.append((at, 1, p, "sum", s))
        at = p + LAG * (len(stages) - 1)
        done.append(max(at, hold + LAG) if late else at)
    for c, members in enumerate(halves_of):
        at = max(done[p] for p in members)
        tasks.append((at, 2, c, "finish", 0))
        tasks.append((at + LAG, 3, c, "inject", 0))
    return sorted(tasks)


def members_of(pieces):
    last = pieces[-1][0]
    return [[p for p, piece in enumerate(pieces) if piece[0] == c] for c in range(last + 1)]


def share_out(table, tasks, members):
    sent, waited, taken = {}, {}, {}
    for at, (_, _, item, what, s) in enumerate(tasks):
        if what == "encode":
            sent[item, 0] = at
        elif what == "sum":
            sent[item, s + 1] = at
            waited[item, s] = at
        elif what == "finish":
            for p in members[item]:
                waited[p, len(table[p]) - 1] = at
    group = {key: tuple(peer for peer, _ in table[key[0]][key[1]][1]) for key in sent}
    last, sem_of = [], {}
    for key in sorted(sent, key=sent.get):
        reply = [k for k in sent if group[k] == group[key] and waited[k] <= sent[key]]
        for sem, old in enumerate(last):
            if group[old] == group[key] and any(waited[old] <= sent[k] for k in reply):
                sem_of[key], last[sem] = sem, key
                break
        else:
            sem_of[key] = len(last)
            last.append(key)
    return sem_of, len(last)


def kernel(dims, pieces, table, tasks, sem_of, shot_hbm, code_hbm, obs_hbm, blk_hbm, idx_hbm, wgt_hbm, out,
           shot, code_ref, obs, blk_ref, idx_ref, wgt_ref, signs, weights, acc, send, recv,
           send3, recv3, left, select, slotm, load_sem, ssem, rsem, s3, r3):
    n, groups, owned, halves = dims
    bits = n.bit_length() - 1
    shots, rcv, _ = shot_hbm.shape
    part = rcv // CUTS
    members = members_of(pieces)
    chunks = owned * halves
    slots = groups * CAP
    me = lax.axis_index("shot")
    mine = lax.axis_index("rcv")

    def partner(mask):
        at = me
        for bit in range(bits):
            if mask >> bit & 1:
                own = lax.rem(lax.div(me, 1 << bit), 2)
                at = at + (1 << bit) - own * (2 << bit)
        return at

    partners = [partner(mask) for mask in range(n)]

    def rcv_peer(e):
        return lax.rem(mine + e, groups)

    def cut(h):
        return pl.ds(h * LANES, LANES)

    small = [(code_hbm, code_ref), (blk_hbm, blk_ref), (idx_hbm, idx_ref), (wgt_hbm, wgt_ref),
             (obs_hbm, obs)]
    small = [pltpu.make_async_copy(src, dst, load_sem.at[i]) for i, (src, dst) in enumerate(small)]
    loads = {}
    for h in range(halves):
        for q in range(CUTS):
            some = pl.ds(q * part, part)
            loads[h, q] = pltpu.make_async_copy(
                shot_hbm.at[:, some, cut(h)], shot.at[h, :, some, :],
                load_sem.at[len(small) + h * CUTS + q])
    small[0].start()
    for load in loads.values():
        load.start()
    for load in small[1:]:
        load.start()

    barrier = pltpu.get_barrier_semaphore()
    near = [1 << bit for bit in range(bits)]
    for mask in near:
        pl.semaphore_signal(barrier, inc=1, device_id={"shot": partners[mask]}, device_id_type=MESH)
    for e in range(1, groups):
        pl.semaphore_signal(barrier, inc=1, device_id={"rcv": rcv_peer(e)}, device_id_type=MESH)

    out_rows, depth = n * ROWS, shots * ROWS
    spread_s = (lax.broadcasted_iota(jnp.int32, (shots, depth), 1)
                - ROWS * lax.broadcasted_iota(jnp.int32, (shots, depth), 0))
    spread_s = ((spread_s >= 0) & (spread_s < ROWS)).astype(F32).astype(BF16)

    def widen(j):
        same_row = ((lax.broadcasted_iota(jnp.int32, (out_rows, depth), 0) & (ROWS - 1))
                    == (lax.broadcasted_iota(jnp.int32, (out_rows, depth), 1) & (ROWS - 1)))
        for m in range(n):
            line = code_ref[pl.ds(partners[m] * owned + j, 1), :].astype(F32)
            signs[j, m * ROWS:(m + 1) * ROWS, :] = jnp.broadcast_to(line, (ROWS, shots)).astype(BF16)
        wide = jnp.dot(signs[j], spread_s, preferred_element_type=F32)
        weights[j] = jnp.where(same_row, wide, 0.0).astype(BF16)

    def copy_of(p, slot, count, sem, peer):
        c, row, rows = pieces[p]
        some = pl.ds(row, rows)
        return pltpu.make_async_remote_copy(
            src_ref=send.at[c, pl.ds(slot, count), some], dst_ref=recv.at[c, pl.ds(slot, count), some],
            send_sem=ssem, recv_sem=rsem.at[sem],
            device_id={"shot": partners[peer]}, device_id_type=MESH)

    def copies(p, s):
        kept, peers, _ = table[p][s]
        return [copy_of(p, slot, len(kept), sem_of[p, s], peer) for peer, slot in peers]

    def wait_for(p, s):
        _, peers, (first, count) = table[p][s]
        copy_of(p, first, count, sem_of[p, s], peers[0][0]).wait_recv()

    def copy3(c, e):
        return pltpu.make_async_remote_copy(
            src_ref=send3.at[c, e - 1], dst_ref=recv3.at[c, e], send_sem=s3,
            recv_sem=r3.at[c], device_id={"rcv": rcv_peer(e)}, device_id_type=MESH)

    def copies3(c):
        return pltpu.make_async_remote_copy(
            src_ref=send3.at[c], dst_ref=recv3.at[c, pl.ds(1, groups - 1)], send_sem=s3,
            recv_sem=r3.at[c], device_id={"rcv": rcv_peer(1)}, device_id_type=MESH)

    def encode(p, _):
        c, row, size = pieces[p]
        j, h = c // halves, c % halves
        if h == 0 and row == 0:
            if j == 0:
                small[0].wait()
            widen(j)
        if j == 0:
            loads[h, row // part].wait()
        kept, peers, _ = table[p][0]

        def tile(g, carry):
            rows = pl.ds(pl.multiple_of(row + g * ROWS, ROWS), ROWS)
            x = shot[h, :, rows, :]
            y = jnp.dot(weights[j], x.reshape(depth, LANES), preferred_element_type=F32)
            y = y.reshape(n, ROWS, LANES)
            for m in kept:
                acc[c, m, rows, :] = y[m]
            for peer, slot in peers:
                for i, m in enumerate(kept):
                    send[c, slot + i, rows, :] = y[m | peer].astype(BF16)
            return carry

        lax.fori_loop(0, size // ROWS, tile, 0, unroll=min(4, size // ROWS))
        if p == 0:
            pl.semaphore_wait(barrier, len(near) + groups - 1)
        for copy in copies(p, 0):
            copy.start()

    def received(p, s, m):
        kept, peers, _ = table[p][s]
        c, row, rows = pieces[p]
        some = pl.ds(row, rows)
        total = acc[c, m, some]
        for _, slot in peers:
            total = total + recv[c, slot + kept.index(m), some].astype(F32)
        return total

    def sum_up(p, s):
        wait_for(p, s)
        kept, peers, _ = table[p][s + 1]
        c, row, rows = pieces[p]
        some = pl.ds(row, rows)
        for (peer, slot), copy in zip(peers, copies(p, s + 1)):
            for i, m in enumerate(kept):
                send[c, slot + i, some] = received(p, s, m | peer).astype(BF16)
            copy.start()
        for m in kept:
            acc[c, m, some] = received(p, s, m)

    def finish(c, _):
        j, h = c // halves, c % halves
        for p in members[c]:
            _, row, rows = pieces[p]
            some = pl.ds(row, rows)
            wait_for(p, len(table[p]) - 1)
            residual = received(p, len(table[p]) - 1, 0) - obs[j, some, cut(h)].astype(F32)
            left[c, some] = residual.astype(BF16)
        picked = jnp.dot(select[...], left[c], preferred_element_type=F32).astype(BF16)
        for e in range(1, groups):
            send3[c, e - 1] = picked[e * CAP:(e + 1) * CAP]
            copy3(c, e).start()
        recv3[c, 0] = picked[:CAP]

    def inject(c, _):
        copies3(c).wait_recv()
        arrived = recv3[c].reshape(slots, LANES)
        j, h = c // halves, c % halves
        out[j, :, cut(h)] = jnp.dot(slotm[...], arrived, preferred_element_type=F32)

    def prepare():
        before = (lax.broadcasted_iota(jnp.int32, (rcv, rcv), 0)
                  < lax.broadcasted_iota(jnp.int32, (rcv, rcv), 1)).astype(F32).astype(BF16)
        slot_at = lax.broadcasted_iota(jnp.int32, (slots, rcv), 0)
        point_at = lax.broadcasted_iota(jnp.int32, (GRID, rcv), 0)
        block_at = lax.broadcasted_iota(jnp.int32, (max(16, groups), rcv), 0)

        def rank_of(ids):
            hot = (block_at == ids).astype(F32)
            count = jnp.dot(hot.astype(BF16), before, preferred_element_type=F32)
            return jnp.sum(hot * count, axis=0, keepdims=True).astype(jnp.int32)

        total = jnp.zeros((GRID, slots), F32)
        for e in range(groups):
            source = lax.rem(mine - e + groups, groups)
            at = pl.ds(pl.multiple_of(source * rcv, rcv), rcv)
            ids = blk_ref[:, at]
            rank = rank_of(ids)
            if e == 0:
                ahead = ids - mine
                ahead = jnp.where(ahead < 0, ahead + groups, ahead)
                select[...] = (slot_at == ahead * CAP + rank).astype(F32).astype(BF16)
            spread = jnp.zeros((GRID, rcv), F32)
            for w in range(idx_ref.shape[0]):
                spread = spread + jnp.where(
                    point_at == idx_ref[pl.ds(w, 1), at], wgt_ref[pl.ds(w, 1), at], 0.0)
            key = jnp.where(ids == mine, e * CAP + rank, -1)
            pick = (slot_at == key).astype(F32).astype(BF16)
            total = total + lax.dot_general(
                spread.astype(BF16), pick, (((1,), (1,)), ((), ())), preferred_element_type=F32)
        slotm[...] = total.astype(BF16)

    act = {"encode": encode, "sum": sum_up, "finish": finish, "inject": inject}
    prepared = False
    for _, _, item, what, s in tasks:
        if what != "encode" and not prepared:
            for load in small[1:]:
                load.wait()
            prepare()
            prepared = True
        act[what](item, s)
    pltpu.make_async_remote_copy(
        src_ref=send, dst_ref=recv, send_sem=ssem, recv_sem=rsem.at[0],
        device_id={"shot": partners[1]}, device_id_type=MESH).wait_send()
    pltpu.make_async_remote_copy(
        src_ref=send3, dst_ref=send3, send_sem=s3, recv_sem=r3.at[0],
        device_id={"rcv": rcv_peer(1)}, device_id_type=MESH).wait_send()


def on_device(n_shot, n_rcv, shot_data, code, observed, block_of, stencil_index, stencil_weight):
    shots, rcv, samples = shot_data.shape
    owned = observed.shape[0]
    halves = samples // LANES
    chunks = owned * halves
    pieces = cut_up(chunks, rcv)
    slots = n_rcv * CAP
    table = plan(len(pieces), n_shot.bit_length() - 1)
    members = members_of(pieces)
    tasks = schedule(table, members)
    sem_of, sems = share_out(table, tasks, members)
    hbm = pl.BlockSpec(memory_space=pltpu.HBM)
    vmem = pltpu.VMEM
    dma = pltpu.SemaphoreType.DMA
    rows = (block_of.T, stencil_index.T, stencil_weight.T)
    return pl.pallas_call(
        functools.partial(kernel, (n_shot, n_rcv, owned, halves), pieces, table, tasks, sem_of),
        out_shape=pltpu.VMEM((owned, GRID, samples), F32),
        in_specs=[hbm] * 6,
        out_specs=pl.BlockSpec(memory_space=vmem),
        scratch_shapes=[
            vmem((halves, shots, rcv, LANES), BF16),
            vmem(code.shape, code.dtype),
            vmem((owned, rcv, samples), BF16),
            *[vmem(row.shape, row.dtype) for row in rows],
            vmem((owned, n_shot * ROWS, shots), BF16),
            vmem((owned, n_shot * ROWS, shots * ROWS), BF16),
            vmem((chunks, n_shot, rcv, LANES), F32),
            vmem((chunks, n_shot - 1, rcv, LANES), BF16),
            vmem((chunks, n_shot - 1, rcv, LANES), BF16),
            vmem((chunks, n_rcv - 1, CAP, LANES), BF16),
            vmem((chunks, n_rcv, CAP, LANES), BF16),
            vmem((chunks, rcv, LANES), BF16),
            vmem((slots, rcv), BF16),
            vmem((GRID, slots), BF16),
            dma((5 + halves * CUTS,)),
            dma,
            dma((sems,)),
            dma,
            dma((chunks,)),
        ],
        compiler_params=pltpu.CompilerParams(
            collective_id=0, has_side_effects=True, vmem_limit_bytes=40 * 2**20),
    )(*[pltpu.with_memory_space_constraint(x, pltpu.HBM)
        for x in (shot_data, code, observed, *rows)])


def solution(mesh):
    placed = (P("shot", "rcv", None), P(None, "shot"), P("shot", "rcv", None), P(), P(), P())
    body = functools.partial(on_device, mesh.shape["shot"], mesh.shape["rcv"])
    return jax.shard_map(
        body, mesh=mesh, in_specs=placed, out_specs=P("shot", "rcv", None), check_vma=False
    )
```

```python
import functools

import jax
import jax.numpy as jnp
from jax import lax
from jax.experimental import pallas as pl
from jax.experimental.pallas import tpu as pltpu
from jax.sharding import PartitionSpec as P

GRID = 256
CAP = 64
ROWS = 16
LANES = 128
CUTS = 4
AHEAD = 4
LAG = 4
HOLD = 3
DIRECT = 4
SPLIT = 0
EARLY = 2
PICK_AT = 3
PICK_STEP = 0.75
INJECT_LAG = 2
LOW_FIRST = 5 / 32
LOW_SPAN = 20 / 32

BF16, F32 = jnp.bfloat16, jnp.float32
MESH = pl.DeviceIdType.MESH


def stages_of(piece, pieces, bits):
    rest = [(bit,) for bit in range(1, bits)]
    low = max(1, round(pieces * LOW_FIRST))
    span = round(pieces * LOW_SPAN)
    if bits == 1:
        return [(0,)]
    if piece >= pieces - DIRECT:
        return [(0,), tuple(range(1, bits))]
    if piece in [1 + i * (span - 1) // low for i in range(low)]:
        return rest + [(0,)]
    return [(0,)] + rest


def cut_up(chunks, rcv):
    part = rcv // CUTS
    pieces = [(c, q * part, part) for c in range(chunks) for q in range(CUTS)]
    for _ in range(SPLIT if part % (2 * ROWS) == 0 else 0):
        c, row, rows = pieces.pop()
        pieces += [(c, row, rows // 2), (c, row + rows // 2, rows // 2)]
    return pieces


def plan(pieces, bits):
    table = []
    for piece in range(pieces):
        left, slot, stages = list(range(1 << bits)), 0, []
        for group in stages_of(piece, pieces, bits):
            mask = sum(1 << bit for bit in group)
            kept = [m for m in left if not m & mask]
            first, peers = slot, []
            for peer in range(1, 1 << bits):
                if not peer & ~mask:
                    peers.append((peer, slot))
                    slot += len(kept)
            stages.append((kept, peers, (first, slot - first)))
            left = kept
        table.append(stages)
    return table


def schedule(table, halves_of, early):
    hold, tasks, done = len(table) - HOLD, [], []
    plain = len(halves_of) - early
    for i in range(early):
        for s in range(CUTS + 3):
            at = PICK_AT + PICK_STEP * (i * (CUTS + 3) + s)
            tasks.append((at, 0, plain + i, "pick", s))
    for p, stages in enumerate(table):
        late = stages[0][1][0][0] != 1
        tasks.append((max(p - AHEAD, -1), 0, p, "encode", 0))
        for s in range(len(stages) - 1):
            at = p + LAG * s
            if late and s == len(stages) - 2:
                at = max(at, hold)
            tasks.append((at, 1, p, "sum", s))
        at = p + LAG * (len(stages) - 1)
        done.append(max(at, hold + LAG) if late else at)
    for c, members in enumerate(halves_of):
        at = max(done[p] for p in members)
        tasks.append((at, 2 if c < plain else 4, c, "finish", 0))
        if c < plain:
            tasks.append((at + INJECT_LAG, 3, c, "inject", 0))
    return sorted(tasks)


def members_of(pieces):
    last = pieces[-1][0]
    return [[p for p, piece in enumerate(pieces) if piece[0] == c] for c in range(last + 1)]


def share_out(table, tasks, members):
    sent, waited, taken = {}, {}, {}
    for at, (_, _, item, what, s) in enumerate(tasks):
        if what == "encode":
            sent[item, 0] = at
        elif what == "sum":
            sent[item, s + 1] = at
            waited[item, s] = at
        elif what == "finish":
            for p in members[item]:
                waited[p, len(table[p]) - 1] = at
    group = {key: tuple(peer for peer, _ in table[key[0]][key[1]][1]) for key in sent}
    last, sem_of = [], {}
    for key in sorted(sent, key=sent.get):
        reply = [k for k in sent if group[k] == group[key] and waited[k] <= sent[key]]
        for sem, old in enumerate(last):
            if group[old] == group[key] and any(waited[old] <= sent[k] for k in reply):
                sem_of[key], last[sem] = sem, key
                break
        else:
            sem_of[key] = len(last)
            last.append(key)
    return sem_of, len(last)


def kernel(dims, pieces, table, tasks, sem_of, shot_hbm, code_hbm, obs_hbm, blk_hbm, idx_hbm, wgt_hbm, out,
           shot, code_ref, obs, blk_ref, idx_ref, wgt_ref, signs, weights, acc, send, recv,
           send3, recv3, left, full, sendx, recvx, select, slotm, load_sem, ssem, rsem, s3, r3, sx, rx):
    n, groups, owned, halves, early = dims
    bits = n.bit_length() - 1
    shots, rcv, _ = shot_hbm.shape
    part = rcv // CUTS
    members = members_of(pieces)
    chunks = owned * halves
    plain = chunks - early
    slots = groups * CAP
    me = lax.axis_index("shot")
    mine = lax.axis_index("rcv")

    def partner(mask):
        at = me
        for bit in range(bits):
            if mask >> bit & 1:
                own = lax.rem(lax.div(me, 1 << bit), 2)
                at = at + (1 << bit) - own * (2 << bit)
        return at

    partners = [partner(mask) for mask in range(n)]

    def rcv_peer(e):
        return lax.rem(mine + e, groups)

    def cut(h):
        return pl.ds(h * LANES, LANES)

    small = [(code_hbm, code_ref), (blk_hbm, blk_ref), (idx_hbm, idx_ref), (wgt_hbm, wgt_ref),
             (obs_hbm, obs)]
    small = [pltpu.make_async_copy(src, dst, load_sem.at[i]) for i, (src, dst) in enumerate(small)]
    loads = {}
    for h in range(halves):
        for q in range(CUTS):
            some = pl.ds(q * part, part)
            loads[h, q] = pltpu.make_async_copy(
                shot_hbm.at[:, some, cut(h)], shot.at[h, :, some, :],
                load_sem.at[len(small) + h * CUTS + q])
    small[0].start()
    for load in loads.values():
        load.start()
    for load in small[1:]:
        load.start()

    barrier = pltpu.get_barrier_semaphore()
    near = [1 << bit for bit in range(bits)]
    for mask in near:
        pl.semaphore_signal(barrier, inc=1, device_id={"shot": partners[mask]}, device_id_type=MESH)
    for e in range(1, groups):
        pl.semaphore_signal(barrier, inc=1, device_id={"rcv": rcv_peer(e)}, device_id_type=MESH)

    out_rows, depth = n * ROWS, shots * ROWS
    spread_s = (lax.broadcasted_iota(jnp.int32, (shots, depth), 1)
                - ROWS * lax.broadcasted_iota(jnp.int32, (shots, depth), 0))
    spread_s = ((spread_s >= 0) & (spread_s < ROWS)).astype(F32).astype(BF16)

    def widen(j):
        same_row = ((lax.broadcasted_iota(jnp.int32, (out_rows, depth), 0) & (ROWS - 1))
                    == (lax.broadcasted_iota(jnp.int32, (out_rows, depth), 1) & (ROWS - 1)))
        for m in range(n):
            line = code_ref[pl.ds(partners[m] * owned + j, 1), :].astype(F32)
            signs[j, m * ROWS:(m + 1) * ROWS, :] = jnp.broadcast_to(line, (ROWS, shots)).astype(BF16)
        wide = jnp.dot(signs[j], spread_s, preferred_element_type=F32)
        weights[j] = jnp.where(same_row, wide, 0.0).astype(BF16)

    def copy_of(p, slot, count, sem, peer):
        c, row, rows = pieces[p]
        some = pl.ds(row, rows)
        return pltpu.make_async_remote_copy(
            src_ref=send.at[c, pl.ds(slot, count), some], dst_ref=recv.at[c, pl.ds(slot, count), some],
            send_sem=ssem, recv_sem=rsem.at[sem],
            device_id={"shot": partners[peer]}, device_id_type=MESH)

    def copies(p, s):
        kept, peers, _ = table[p][s]
        return [copy_of(p, slot, len(kept), sem_of[p, s], peer) for peer, slot in peers]

    def wait_for(p, s):
        _, peers, (first, count) = table[p][s]
        copy_of(p, first, count, sem_of[p, s], peers[0][0]).wait_recv()

    def copy3(c, e):
        return pltpu.make_async_remote_copy(
            src_ref=send3.at[c, e - 1], dst_ref=recv3.at[c, e], send_sem=s3,
            recv_sem=r3.at[c], device_id={"rcv": rcv_peer(e)}, device_id_type=MESH)

    def copies3(c):
        return pltpu.make_async_remote_copy(
            src_ref=send3.at[c], dst_ref=recv3.at[c, pl.ds(1, groups - 1)], send_sem=s3,
            recv_sem=r3.at[c], device_id={"rcv": rcv_peer(1)}, device_id_type=MESH)

    def copyx(i, e):
        return pltpu.make_async_remote_copy(
            src_ref=sendx.at[i, e - 1], dst_ref=recvx.at[i, e], send_sem=sx,
            recv_sem=rx.at[i], device_id={"rcv": rcv_peer(e)}, device_id_type=MESH)

    def copiesx(i):
        return pltpu.make_async_remote_copy(
            src_ref=sendx.at[i], dst_ref=recvx.at[i, pl.ds(1, groups - 1)], send_sem=sx,
            recv_sem=rx.at[i], device_id={"rcv": rcv_peer(1)}, device_id_type=MESH)

    widened = set()

    def mix(c, row, size, put):
        j, h = c // halves, c % halves
        if j not in widened:
            if not widened:
                small[0].wait()
            widened.add(j)
            widen(j)
        if j == 0:
            loads[h, row // part].wait()

        def tile(g, carry):
            rows = pl.ds(pl.multiple_of(row + g * ROWS, ROWS), ROWS)
            x = shot[h, :, rows, :]
            y = jnp.dot(weights[j], x.reshape(depth, LANES), preferred_element_type=F32)
            put(rows, y.reshape(n, ROWS, LANES))
            return carry

        lax.fori_loop(0, size // ROWS, tile, 0, unroll=min(4, size // ROWS))

    def pick(c, s):
        i, j, h = c - plain, c // halves, c % halves
        if s < CUTS:
            def put(rows, y):
                full[:, rows, :] = y.astype(BF16)

            mix(c, s * part, part, put)
            return
        third = -(-(n + 1) // 3)
        for m in range((s - CUTS) * third, min(n + 1, (s - CUTS + 1) * third)):
            rows = full[m] if m < n else obs[j, :, cut(h)]
            picked = jnp.dot(select[...], rows, preferred_element_type=F32).astype(BF16)
            recvx[i, 0, m] = picked[:CAP]
            for e in range(1, groups):
                sendx[i, e - 1, m] = picked[e * CAP:(e + 1) * CAP]
        if s == CUTS + 2:
            for e in range(1, groups):
                copyx(i, e).start()

    def encode(p, _):
        c, row, size = pieces[p]
        kept, peers, _ = table[p][0]
        if c >= plain:
            i, e, some = c - plain, row // CAP, pl.ds(row, size)
            if row == 0:
                copiesx(i).wait_recv()
            for m in kept:
                acc[c, m, some] = recvx[i, e, m].astype(F32)
            for peer, slot in peers:
                for k, m in enumerate(kept):
                    send[c, slot + k, some] = recvx[i, e, m | peer]
        else:
            def put(rows, y):
                for m in kept:
                    acc[c, m, rows, :] = y[m]
                for peer, slot in peers:
                    for i, m in enumerate(kept):
                        send[c, slot + i, rows, :] = y[m | peer].astype(BF16)

            mix(c, row, size, put)
        if p == 0:
            pl.semaphore_wait(barrier, len(near) + groups - 1)
        for copy in copies(p, 0):
            copy.start()

    def received(p, s, m):
        kept, peers, _ = table[p][s]
        c, row, rows = pieces[p]
        some = pl.ds(row, rows)
        total = acc[c, m, some]
        for _, slot in peers:
            total = total + recv[c, slot + kept.index(m), some].astype(F32)
        return total

    def sum_up(p, s):
        wait_for(p, s)
        kept, peers, _ = table[p][s + 1]
        c, row, rows = pieces[p]
        some = pl.ds(row, rows)
        for (peer, slot), copy in zip(peers, copies(p, s + 1)):
            for i, m in enumerate(kept):
                send[c, slot + i, some] = received(p, s, m | peer).astype(BF16)
            copy.start()
        for m in kept:
            acc[c, m, some] = received(p, s, m)

    def finish(c, _):
        j, h = c // halves, c % halves
        for p in members[c]:
            _, row, rows = pieces[p]
            some = pl.ds(row, rows)
            wait_for(p, len(table[p]) - 1)
            seen = obs[j, some, cut(h)] if c < plain else recvx[c - plain, row // CAP, n]
            residual = received(p, len(table[p]) - 1, 0) - seen.astype(F32)
            left[c, some] = residual.astype(BF16)
        if c >= plain:
            out[j, :, cut(h)] = jnp.dot(slotm[...], left[c], preferred_element_type=F32)
            return
        picked = jnp.dot(select[...], left[c], preferred_element_type=F32).astype(BF16)
        for e in range(1, groups):
            send3[c, e - 1] = picked[e * CAP:(e + 1) * CAP]
            copy3(c, e).start()
        recv3[c, 0] = picked[:CAP]

    def inject(c, _):
        copies3(c).wait_recv()
        arrived = recv3[c].reshape(slots, LANES)
        j, h = c // halves, c % halves
        out[j, :, cut(h)] = jnp.dot(slotm[...], arrived, preferred_element_type=F32)

    def prepare():
        before = (lax.broadcasted_iota(jnp.int32, (rcv, rcv), 0)
                  < lax.broadcasted_iota(jnp.int32, (rcv, rcv), 1)).astype(F32).astype(BF16)
        slot_at = lax.broadcasted_iota(jnp.int32, (slots, rcv), 0)
        point_at = lax.broadcasted_iota(jnp.int32, (GRID, rcv), 0)
        block_at = lax.broadcasted_iota(jnp.int32, (max(16, groups), rcv), 0)

        def rank_of(ids):
            hot = (block_at == ids).astype(F32)
            count = jnp.dot(hot.astype(BF16), before, preferred_element_type=F32)
            return jnp.sum(hot * count, axis=0, keepdims=True).astype(jnp.int32)

        total = jnp.zeros((GRID, slots), F32)
        for e in range(groups):
            source = lax.rem(mine - e + groups, groups)
            at = pl.ds(pl.multiple_of(source * rcv, rcv), rcv)
            ids = blk_ref[:, at]
            rank = rank_of(ids)
            if e == 0:
                ahead = ids - mine
                ahead = jnp.where(ahead < 0, ahead + groups, ahead)
                select[...] = (slot_at == ahead * CAP + rank).astype(F32).astype(BF16)
            spread = jnp.zeros((GRID, rcv), F32)
            for w in range(idx_ref.shape[0]):
                spread = spread + jnp.where(
                    point_at == idx_ref[pl.ds(w, 1), at], wgt_ref[pl.ds(w, 1), at], 0.0)
            key = jnp.where(ids == mine, e * CAP + rank, -1)
            pick = (slot_at == key).astype(F32).astype(BF16)
            total = total + lax.dot_general(
                spread.astype(BF16), pick, (((1,), (1,)), ((), ())), preferred_element_type=F32)
        slotm[...] = total.astype(BF16)

    act = {"pick": pick, "encode": encode, "sum": sum_up, "finish": finish, "inject": inject}
    prepared = False
    for _, _, item, what, s in tasks:
        if what != "encode" and not prepared:
            for load in small[1:]:
                load.wait()
            prepare()
            prepared = True
        act[what](item, s)
    pltpu.make_async_remote_copy(
        src_ref=send, dst_ref=recv, send_sem=ssem, recv_sem=rsem.at[0],
        device_id={"shot": partners[1]}, device_id_type=MESH).wait_send()
    pltpu.make_async_remote_copy(
        src_ref=send3, dst_ref=send3, send_sem=s3, recv_sem=r3.at[0],
        device_id={"rcv": rcv_peer(1)}, device_id_type=MESH).wait_send()
    if early:
        pltpu.make_async_remote_copy(
            src_ref=sendx, dst_ref=sendx, send_sem=sx, recv_sem=rx.at[0],
            device_id={"rcv": rcv_peer(1)}, device_id_type=MESH).wait_send()


def on_device(n_shot, n_rcv, shot_data, code, observed, block_of, stencil_index, stencil_weight):
    shots, rcv, samples = shot_data.shape
    owned = observed.shape[0]
    halves = samples // LANES
    chunks = owned * halves
    pieces = cut_up(chunks, rcv)
    slots = n_rcv * CAP
    part = rcv // CUTS
    table = plan(len(pieces), n_shot.bit_length() - 1)
    members = members_of(pieces)
    early = EARLY if slots == rcv and part == CAP and SPLIT == 0 else 0
    tasks = schedule(table, members, early)
    kinds = max(early, 1)
    plain = chunks - early
    sem_of, sems = share_out(table, tasks, members)
    hbm = pl.BlockSpec(memory_space=pltpu.HBM)
    vmem = pltpu.VMEM
    dma = pltpu.SemaphoreType.DMA
    rows = (block_of.T, stencil_index.T, stencil_weight.T)
    return pl.pallas_call(
        functools.partial(kernel, (n_shot, n_rcv, owned, halves, early), pieces, table, tasks, sem_of),
        out_shape=pltpu.VMEM((owned, GRID, samples), F32),
        in_specs=[hbm] * 6,
        out_specs=pl.BlockSpec(memory_space=vmem),
        scratch_shapes=[
            vmem((halves, shots, rcv, LANES), BF16),
            vmem(code.shape, code.dtype),
            vmem((owned, rcv, samples), BF16),
            *[vmem(row.shape, row.dtype) for row in rows],
            vmem((owned, n_shot * ROWS, shots), BF16),
            vmem((owned, n_shot * ROWS, shots * ROWS), BF16),
            vmem((chunks, n_shot, rcv, LANES), F32),
            vmem((chunks, n_shot - 1, rcv, LANES), BF16),
            vmem((chunks, n_shot - 1, rcv, LANES), BF16),
            vmem((plain, n_rcv - 1, CAP, LANES), BF16),
            vmem((plain, n_rcv, CAP, LANES), BF16),
            vmem((chunks, rcv, LANES), BF16),
            vmem((n_shot, rcv, LANES), BF16),
            vmem((kinds, n_rcv - 1, n_shot + 1, CAP, LANES), BF16),
            vmem((kinds, n_rcv, n_shot + 1, CAP, LANES), BF16),
            vmem((slots, rcv), BF16),
            vmem((GRID, slots), BF16),
            dma((5 + halves * CUTS,)),
            dma,
            dma((sems,)),
            dma,
            dma((plain,)),
            dma,
            dma((kinds,)),
        ],
        compiler_params=pltpu.CompilerParams(
            collective_id=0, has_side_effects=True, vmem_limit_bytes=40 * 2**20),
    )(*[pltpu.with_memory_space_constraint(x, pltpu.HBM)
        for x in (shot_data, code, observed, *rows)])


def solution(mesh):
    placed = (P("shot", "rcv", None), P(None, "shot"), P("shot", "rcv", None), P(), P(), P())
    body = functools.partial(on_device, mesh.shape["shot"], mesh.shape["rcv"])
    return jax.shard_map(
        body, mesh=mesh, in_specs=placed, out_specs=P("shot", "rcv", None), check_vma=False
    )
```

```python
import functools

import jax
import jax.numpy as jnp
from jax import lax
from jax.experimental import pallas as pl
from jax.experimental.pallas import tpu as pltpu
from jax.sharding import PartitionSpec as P

GRID = 256
CAP = 64
ROWS = 16
LANES = 128
CUTS = 4
AHEAD = 4
LAG = 4
HOLD = 3
DIRECT = 4
SPLIT = 0
EARLY = 2
PICK_AT = 3
PICK_STEP = 0.75
INJECT_LAG = 2
SOONER = 0.5
LATER = 0.25
LOW_FIRST = 5 / 32
LOW_SPAN = 20 / 32

BF16, F32 = jnp.bfloat16, jnp.float32
MESH = pl.DeviceIdType.MESH


def stages_of(piece, pieces, bits):
    rest = [(bit,) for bit in range(1, bits)]
    low = max(1, round(pieces * LOW_FIRST))
    span = round(pieces * LOW_SPAN)
    if bits == 1:
        return [(0,)]
    if piece >= pieces - DIRECT:
        return [(0,), tuple(range(1, bits))]
    if piece in [1 + i * (span - 1) // low for i in range(low)]:
        return rest + [(0,)]
    return [(0,)] + rest


def cut_up(chunks, rcv):
    part = rcv // CUTS
    pieces = [(c, q * part, part) for c in range(chunks) for q in range(CUTS)]
    for _ in range(SPLIT if part % (2 * ROWS) == 0 else 0):
        c, row, rows = pieces.pop()
        pieces += [(c, row, rows // 2), (c, row + rows // 2, rows // 2)]
    return pieces


def plan(pieces, bits):
    table = []
    for piece in range(pieces):
        left, slot, stages = list(range(1 << bits)), 0, []
        for group in stages_of(piece, pieces, bits):
            mask = sum(1 << bit for bit in group)
            kept = [m for m in left if not m & mask]
            first, peers = slot, []
            for peer in range(1, 1 << bits):
                if not peer & ~mask:
                    peers.append((peer, slot))
                    slot += len(kept)
            stages.append((kept, peers, (first, slot - first)))
            left = kept
        table.append(stages)
    return table


def schedule(table, halves_of, early):
    hold, tasks, done = len(table) - HOLD, [], []
    plain = len(halves_of) - early
    for i in range(early):
        for s in range(CUTS + 3):
            at = PICK_AT + PICK_STEP * (i * (CUTS + 3) + s)
            tasks.append((at, 0, plain + i, "pick", s))
    for p, stages in enumerate(table):
        late = stages[0][1][0][0] != 1
        tasks.append((max(p - AHEAD, -1), 0, p, "encode", 0))
        for s in range(len(stages) - 1):
            at = p + LAG * s
            if late and s == len(stages) - 2:
                at = max(at, hold)
            tasks.append((at, 1, p, "sum", s))
        at = p + LAG * (len(stages) - 1)
        done.append(max(at, hold + LAG) if late else at)
    for c, members in enumerate(halves_of):
        at = max(done[p] for p in members)
        if c < plain:
            at -= SOONER if at < hold + LAG else 0
            tasks.append((at, 2, c, "finish", 0))
            inject = max(at + INJECT_LAG, hold + LAG + 0.5)
            tasks.append((inject + 0.1 * c, 3, c, "inject", 0))
        else:
            tasks.append((at + LATER, 4, c, "finish", 0))
    return sorted(tasks)


def members_of(pieces):
    last = pieces[-1][0]
    return [[p for p, piece in enumerate(pieces) if piece[0] == c] for c in range(last + 1)]


def share_out(table, tasks, members):
    sent, waited, taken = {}, {}, {}
    for at, (_, _, item, what, s) in enumerate(tasks):
        if what == "encode":
            sent[item, 0] = at
        elif what == "sum":
            sent[item, s + 1] = at
            waited[item, s] = at
        elif what == "finish":
            for p in members[item]:
                waited[p, len(table[p]) - 1] = at
    group = {key: tuple(peer for peer, _ in table[key[0]][key[1]][1]) for key in sent}
    last, sem_of = [], {}
    for key in sorted(sent, key=sent.get):
        reply = [k for k in sent if group[k] == group[key] and waited[k] <= sent[key]]
        for sem, old in enumerate(last):
            if group[old] == group[key] and any(waited[old] <= sent[k] for k in reply):
                sem_of[key], last[sem] = sem, key
                break
        else:
            sem_of[key] = len(last)
            last.append(key)
    return sem_of, len(last)


def kernel(dims, pieces, table, tasks, sem_of, shot_hbm, code_hbm, obs_hbm, blk_hbm, idx_hbm, wgt_hbm, out,
           shot, code_ref, obs, blk_ref, idx_ref, wgt_ref, signs, weights, acc, send, recv,
           send3, recv3, left, full, sendx, recvx, select, slotm, load_sem, ssem, rsem, s3, r3, sx, rx):
    n, groups, owned, halves, early = dims
    bits = n.bit_length() - 1
    shots, rcv, _ = shot_hbm.shape
    part = rcv // CUTS
    members = members_of(pieces)
    chunks = owned * halves
    plain = chunks - early
    slots = groups * CAP
    me = lax.axis_index("shot")
    mine = lax.axis_index("rcv")

    def partner(mask):
        at = me
        for bit in range(bits):
            if mask >> bit & 1:
                own = lax.rem(lax.div(me, 1 << bit), 2)
                at = at + (1 << bit) - own * (2 << bit)
        return at

    partners = [partner(mask) for mask in range(n)]

    def rcv_peer(e):
        return lax.rem(mine + e, groups)

    def cut(h):
        return pl.ds(h * LANES, LANES)

    small = [(code_hbm, code_ref), (blk_hbm, blk_ref), (idx_hbm, idx_ref), (wgt_hbm, wgt_ref),
             (obs_hbm, obs)]
    small = [pltpu.make_async_copy(src, dst, load_sem.at[i]) for i, (src, dst) in enumerate(small)]
    loads = {}
    for h in range(halves):
        for q in range(CUTS):
            some = pl.ds(q * part, part)
            loads[h, q] = pltpu.make_async_copy(
                shot_hbm.at[:, some, cut(h)], shot.at[h, :, some, :],
                load_sem.at[len(small) + h * CUTS + q])
    small[0].start()
    for load in loads.values():
        load.start()
    for load in small[1:]:
        load.start()

    barrier = pltpu.get_barrier_semaphore()
    near = [1 << bit for bit in range(bits)]
    for mask in near:
        pl.semaphore_signal(barrier, inc=1, device_id={"shot": partners[mask]}, device_id_type=MESH)
    for e in range(1, groups):
        pl.semaphore_signal(barrier, inc=1, device_id={"rcv": rcv_peer(e)}, device_id_type=MESH)

    out_rows, depth = n * ROWS, shots * ROWS
    spread_s = (lax.broadcasted_iota(jnp.int32, (shots, depth), 1)
                - ROWS * lax.broadcasted_iota(jnp.int32, (shots, depth), 0))
    spread_s = ((spread_s >= 0) & (spread_s < ROWS)).astype(F32).astype(BF16)

    def widen(j):
        same_row = ((lax.broadcasted_iota(jnp.int32, (out_rows, depth), 0) & (ROWS - 1))
                    == (lax.broadcasted_iota(jnp.int32, (out_rows, depth), 1) & (ROWS - 1)))
        for m in range(n):
            line = code_ref[pl.ds(partners[m] * owned + j, 1), :].astype(F32)
            signs[j, m * ROWS:(m + 1) * ROWS, :] = jnp.broadcast_to(line, (ROWS, shots)).astype(BF16)
        wide = jnp.dot(signs[j], spread_s, preferred_element_type=F32)
        weights[j] = jnp.where(same_row, wide, 0.0).astype(BF16)

    def copy_of(p, slot, count, sem, peer):
        c, row, rows = pieces[p]
        some = pl.ds(row, rows)
        return pltpu.make_async_remote_copy(
            src_ref=send.at[c, pl.ds(slot, count), some], dst_ref=recv.at[c, pl.ds(slot, count), some],
            send_sem=ssem, recv_sem=rsem.at[sem],
            device_id={"shot": partners[peer]}, device_id_type=MESH)

    def copies(p, s):
        kept, peers, _ = table[p][s]
        return [copy_of(p, slot, len(kept), sem_of[p, s], peer) for peer, slot in peers]

    def wait_for(p, s):
        _, peers, (first, count) = table[p][s]
        copy_of(p, first, count, sem_of[p, s], peers[0][0]).wait_recv()

    def copy3(c, e):
        return pltpu.make_async_remote_copy(
            src_ref=send3.at[c, e - 1], dst_ref=recv3.at[c, e], send_sem=s3,
            recv_sem=r3.at[c], device_id={"rcv": rcv_peer(e)}, device_id_type=MESH)

    def copies3(c):
        return pltpu.make_async_remote_copy(
            src_ref=send3.at[c], dst_ref=recv3.at[c, pl.ds(1, groups - 1)], send_sem=s3,
            recv_sem=r3.at[c], device_id={"rcv": rcv_peer(1)}, device_id_type=MESH)

    def copyx(i, e):
        return pltpu.make_async_remote_copy(
            src_ref=sendx.at[i, e - 1], dst_ref=recvx.at[i, e], send_sem=sx,
            recv_sem=rx.at[i], device_id={"rcv": rcv_peer(e)}, device_id_type=MESH)

    def copiesx(i):
        return pltpu.make_async_remote_copy(
            src_ref=sendx.at[i], dst_ref=recvx.at[i, pl.ds(1, groups - 1)], send_sem=sx,
            recv_sem=rx.at[i], device_id={"rcv": rcv_peer(1)}, device_id_type=MESH)

    widened = set()

    def mix(c, row, size, put):
        j, h = c // halves, c % halves
        if j not in widened:
            if not widened:
                small[0].wait()
            widened.add(j)
            widen(j)
        if j == 0:
            loads[h, row // part].wait()

        def tile(g, carry):
            rows = pl.ds(pl.multiple_of(row + g * ROWS, ROWS), ROWS)
            x = shot[h, :, rows, :]
            y = jnp.dot(weights[j], x.reshape(depth, LANES), preferred_element_type=F32)
            put(rows, y.reshape(n, ROWS, LANES))
            return carry

        lax.fori_loop(0, size // ROWS, tile, 0, unroll=min(4, size // ROWS))

    def pick(c, s):
        i, j, h = c - plain, c // halves, c % halves
        if s < CUTS:
            def put(rows, y):
                full[:, rows, :] = y.astype(BF16)

            mix(c, s * part, part, put)
            return
        third = -(-(n + 1) // 3)
        for m in range((s - CUTS) * third, min(n + 1, (s - CUTS + 1) * third)):
            rows = full[m] if m < n else obs[j, :, cut(h)]
            picked = jnp.dot(select[...], rows, preferred_element_type=F32).astype(BF16)
            recvx[i, 0, m] = picked[:CAP]
            for e in range(1, groups):
                sendx[i, e - 1, m] = picked[e * CAP:(e + 1) * CAP]
        if s == CUTS + 2:
            for e in range(1, groups):
                copyx(i, e).start()

    def encode(p, _):
        c, row, size = pieces[p]
        kept, peers, _ = table[p][0]
        if c >= plain:
            i, e, some = c - plain, row // CAP, pl.ds(row, size)
            if row == 0:
                copiesx(i).wait_recv()
            for m in kept:
                acc[c, m, some] = recvx[i, e, m].astype(F32)
            for peer, slot in peers:
                for k, m in enumerate(kept):
                    send[c, slot + k, some] = recvx[i, e, m | peer]
        else:
            def put(rows, y):
                for m in kept:
                    acc[c, m, rows, :] = y[m]
                for peer, slot in peers:
                    for i, m in enumerate(kept):
                        send[c, slot + i, rows, :] = y[m | peer].astype(BF16)

            mix(c, row, size, put)
        if p == 0:
            pl.semaphore_wait(barrier, len(near) + groups - 1)
        for copy in copies(p, 0):
            copy.start()

    def received(p, s, m):
        kept, peers, _ = table[p][s]
        c, row, rows = pieces[p]
        some = pl.ds(row, rows)
        total = acc[c, m, some]
        for _, slot in peers:
            total = total + recv[c, slot + kept.index(m), some].astype(F32)
        return total

    def sum_up(p, s):
        wait_for(p, s)
        kept, peers, _ = table[p][s + 1]
        c, row, rows = pieces[p]
        some = pl.ds(row, rows)
        for (peer, slot), copy in zip(peers, copies(p, s + 1)):
            for i, m in enumerate(kept):
                send[c, slot + i, some] = received(p, s, m | peer).astype(BF16)
            copy.start()
        for m in kept:
            acc[c, m, some] = received(p, s, m)

    def finish(c, _):
        j, h = c // halves, c % halves
        for p in members[c]:
            _, row, rows = pieces[p]
            some = pl.ds(row, rows)
            wait_for(p, len(table[p]) - 1)
            seen = obs[j, some, cut(h)] if c < plain else recvx[c - plain, row // CAP, n]
            residual = received(p, len(table[p]) - 1, 0) - seen.astype(F32)
            left[c, some] = residual.astype(BF16)
        if c >= plain:
            out[j, :, cut(h)] = jnp.dot(slotm[...], left[c], preferred_element_type=F32)
            return
        picked = jnp.dot(select[...], left[c], preferred_element_type=F32).astype(BF16)
        for e in range(1, groups):
            send3[c, e - 1] = picked[e * CAP:(e + 1) * CAP]
            copy3(c, e).start()
        recv3[c, 0] = picked[:CAP]

    def inject(c, _):
        copies3(c).wait_recv()
        arrived = recv3[c].reshape(slots, LANES)
        j, h = c // halves, c % halves
        out[j, :, cut(h)] = jnp.dot(slotm[...], arrived, preferred_element_type=F32)

    def prepare():
        before = (lax.broadcasted_iota(jnp.int32, (rcv, rcv), 0)
                  < lax.broadcasted_iota(jnp.int32, (rcv, rcv), 1)).astype(F32).astype(BF16)
        slot_at = lax.broadcasted_iota(jnp.int32, (slots, rcv), 0)
        point_at = lax.broadcasted_iota(jnp.int32, (GRID, rcv), 0)
        block_at = lax.broadcasted_iota(jnp.int32, (max(16, groups), rcv), 0)

        def rank_of(ids):
            hot = (block_at == ids).astype(F32)
            count = jnp.dot(hot.astype(BF16), before, preferred_element_type=F32)
            return jnp.sum(hot * count, axis=0, keepdims=True).astype(jnp.int32)

        total = jnp.zeros((GRID, slots), F32)
        for e in range(groups):
            source = lax.rem(mine - e + groups, groups)
            at = pl.ds(pl.multiple_of(source * rcv, rcv), rcv)
            ids = blk_ref[:, at]
            rank = rank_of(ids)
            if e == 0:
                ahead = ids - mine
                ahead = jnp.where(ahead < 0, ahead + groups, ahead)
                select[...] = (slot_at == ahead * CAP + rank).astype(F32).astype(BF16)
            spread = jnp.zeros((GRID, rcv), F32)
            for w in range(idx_ref.shape[0]):
                spread = spread + jnp.where(
                    point_at == idx_ref[pl.ds(w, 1), at], wgt_ref[pl.ds(w, 1), at], 0.0)
            key = jnp.where(ids == mine, e * CAP + rank, -1)
            pick = (slot_at == key).astype(F32).astype(BF16)
            total = total + lax.dot_general(
                spread.astype(BF16), pick, (((1,), (1,)), ((), ())), preferred_element_type=F32)
        slotm[...] = total.astype(BF16)

    act = {"pick": pick, "encode": encode, "sum": sum_up, "finish": finish, "inject": inject}
    prepared = False
    for _, _, item, what, s in tasks:
        if what != "encode" and not prepared:
            for load in small[1:]:
                load.wait()
            prepare()
            prepared = True
        act[what](item, s)
    pltpu.make_async_remote_copy(
        src_ref=send, dst_ref=recv, send_sem=ssem, recv_sem=rsem.at[0],
        device_id={"shot": partners[1]}, device_id_type=MESH).wait_send()
    pltpu.make_async_remote_copy(
        src_ref=send3, dst_ref=send3, send_sem=s3, recv_sem=r3.at[0],
        device_id={"rcv": rcv_peer(1)}, device_id_type=MESH).wait_send()
    if early:
        pltpu.make_async_remote_copy(
            src_ref=sendx, dst_ref=sendx, send_sem=sx, recv_sem=rx.at[0],
            device_id={"rcv": rcv_peer(1)}, device_id_type=MESH).wait_send()


def on_device(n_shot, n_rcv, shot_data, code, observed, block_of, stencil_index, stencil_weight):
    shots, rcv, samples = shot_data.shape
    owned = observed.shape[0]
    halves = samples // LANES
    chunks = owned * halves
    pieces = cut_up(chunks, rcv)
    slots = n_rcv * CAP
    part = rcv // CUTS
    table = plan(len(pieces), n_shot.bit_length() - 1)
    members = members_of(pieces)
    early = EARLY if slots == rcv and part == CAP and SPLIT == 0 else 0
    tasks = schedule(table, members, early)
    kinds = max(early, 1)
    plain = chunks - early
    sem_of, sems = share_out(table, tasks, members)
    hbm = pl.BlockSpec(memory_space=pltpu.HBM)
    vmem = pltpu.VMEM
    dma = pltpu.SemaphoreType.DMA
    rows = (block_of.T, stencil_index.T, stencil_weight.T)
    return pl.pallas_call(
        functools.partial(kernel, (n_shot, n_rcv, owned, halves, early), pieces, table, tasks, sem_of),
        out_shape=pltpu.VMEM((owned, GRID, samples), F32),
        in_specs=[hbm] * 6,
        out_specs=pl.BlockSpec(memory_space=vmem),
        scratch_shapes=[
            vmem((halves, shots, rcv, LANES), BF16),
            vmem(code.shape, code.dtype),
            vmem((owned, rcv, samples), BF16),
            *[vmem(row.shape, row.dtype) for row in rows],
            vmem((owned, n_shot * ROWS, shots), BF16),
            vmem((owned, n_shot * ROWS, shots * ROWS), BF16),
            vmem((chunks, n_shot, rcv, LANES), F32),
            vmem((chunks, n_shot - 1, rcv, LANES), BF16),
            vmem((chunks, n_shot - 1, rcv, LANES), BF16),
            vmem((plain, n_rcv - 1, CAP, LANES), BF16),
            vmem((plain, n_rcv, CAP, LANES), BF16),
            vmem((chunks, rcv, LANES), BF16),
            vmem((n_shot, rcv, LANES), BF16),
            vmem((kinds, n_rcv - 1, n_shot + 1, CAP, LANES), BF16),
            vmem((kinds, n_rcv, n_shot + 1, CAP, LANES), BF16),
            vmem((slots, rcv), BF16),
            vmem((GRID, slots), BF16),
            dma((5 + halves * CUTS,)),
            dma,
            dma((sems,)),
            dma,
            dma((plain,)),
            dma,
            dma((kinds,)),
        ],
        compiler_params=pltpu.CompilerParams(
            collective_id=0, has_side_effects=True, vmem_limit_bytes=40 * 2**20),
    )(*[pltpu.with_memory_space_constraint(x, pltpu.HBM)
        for x in (shot_data, code, observed, *rows)])


def solution(mesh):
    placed = (P("shot", "rcv", None), P(None, "shot"), P("shot", "rcv", None), P(), P(), P())
    body = functools.partial(on_device, mesh.shape["shot"], mesh.shape["rcv"])
    return jax.shard_map(
        body, mesh=mesh, in_specs=placed, out_specs=P("shot", "rcv", None), check_vma=False
    )
```

```python
import functools

import jax
import jax.numpy as jnp
from jax import lax
from jax.experimental import pallas as pl
from jax.experimental.pallas import tpu as pltpu
from jax.sharding import PartitionSpec as P

GRID = 256
CAP = 64
ROWS = 16
LANES = 128
CUTS = 4
AHEAD = 4
LAG = 4
HOLD = 4
DIRECT = 4
SPLIT = 0
EARLY = 3
PICK_AT = 3
PICK_STEP = 0.75
INJECT_LAG = 2
SOONER = 0.5
LATER = 0.25
LOW_FIRST = 5 / 32
LOW_SPAN = 20 / 32

BF16, F32 = jnp.bfloat16, jnp.float32
MESH = pl.DeviceIdType.MESH


def stages_of(piece, pieces, bits):
    rest = [(bit,) for bit in range(1, bits)]
    low = max(1, round(pieces * LOW_FIRST))
    span = round(pieces * LOW_SPAN)
    if bits == 1:
        return [(0,)]
    if piece >= pieces - DIRECT:
        return [(0,), tuple(range(1, bits))]
    if piece in [1 + i * (span - 1) // low for i in range(low)]:
        return rest + [(0,)]
    return [(0,)] + rest


def cut_up(chunks, rcv):
    part = rcv // CUTS
    pieces = [(c, q * part, part) for c in range(chunks) for q in range(CUTS)]
    for _ in range(SPLIT if part % (2 * ROWS) == 0 else 0):
        c, row, rows = pieces.pop()
        pieces += [(c, row, rows // 2), (c, row + rows // 2, rows // 2)]
    return pieces


def plan(pieces, bits):
    table = []
    for piece in range(pieces):
        left, slot, stages = list(range(1 << bits)), 0, []
        for group in stages_of(piece, pieces, bits):
            mask = sum(1 << bit for bit in group)
            kept = [m for m in left if not m & mask]
            first, peers = slot, []
            for peer in range(1, 1 << bits):
                if not peer & ~mask:
                    peers.append((peer, slot))
                    slot += len(kept)
            stages.append((kept, peers, (first, slot - first)))
            left = kept
        table.append(stages)
    return table


def schedule(table, halves_of, early):
    hold, tasks, done = len(table) - HOLD, [], []
    plain = len(halves_of) - early
    for i in range(early):
        for s in range(CUTS + 3):
            at = PICK_AT + PICK_STEP * (i * (CUTS + 3) + s)
            tasks.append((at, 0, plain + i, "pick", s))
    for p, stages in enumerate(table):
        late = stages[0][1][0][0] != 1
        tasks.append((max(p - AHEAD, -1), 0, p, "encode", 0))
        for s in range(len(stages) - 1):
            at = p + LAG * s
            if late and s == len(stages) - 2:
                at = max(at, hold)
            tasks.append((at, 1, p, "sum", s))
        at = p + LAG * (len(stages) - 1)
        done.append(max(at, hold + LAG) if late else at)
    for c, members in enumerate(halves_of):
        at = max(done[p] for p in members)
        if c < plain:
            at -= SOONER if at < hold + LAG else 0
            tasks.append((at, 2, c, "finish", 0))
            inject = max(at + INJECT_LAG, hold + LAG + 0.5)
            tasks.append((inject + 0.1 * c, 3, c, "inject", 0))
        else:
            tasks.append((at + LATER, 4, c, "finish", 0))
    return sorted(tasks)


def members_of(pieces):
    last = pieces[-1][0]
    return [[p for p, piece in enumerate(pieces) if piece[0] == c] for c in range(last + 1)]


def share_out(table, tasks, members):
    sent, waited, taken = {}, {}, {}
    for at, (_, _, item, what, s) in enumerate(tasks):
        if what == "encode":
            sent[item, 0] = at
        elif what == "sum":
            sent[item, s + 1] = at
            waited[item, s] = at
        elif what == "finish":
            for p in members[item]:
                waited[p, len(table[p]) - 1] = at
    group = {key: tuple(peer for peer, _ in table[key[0]][key[1]][1]) for key in sent}
    last, sem_of = [], {}
    for key in sorted(sent, key=sent.get):
        reply = [k for k in sent if group[k] == group[key] and waited[k] <= sent[key]]
        for sem, old in enumerate(last):
            if group[old] == group[key] and any(waited[old] <= sent[k] for k in reply):
                sem_of[key], last[sem] = sem, key
                break
        else:
            sem_of[key] = len(last)
            last.append(key)
    return sem_of, len(last)


def kernel(dims, pieces, table, tasks, sem_of, shot_hbm, code_hbm, obs_hbm, blk_hbm, idx_hbm, wgt_hbm, out,
           shot, code_ref, obs, blk_ref, idx_ref, wgt_ref, signs, weights, acc, send, recv,
           send3, recv3, left, full, sendx, recvx, select, slotm, load_sem, ssem, rsem, s3, r3, sx, rx):
    n, groups, owned, halves, early = dims
    bits = n.bit_length() - 1
    shots, rcv, _ = shot_hbm.shape
    part = rcv // CUTS
    members = members_of(pieces)
    chunks = owned * halves
    plain = chunks - early
    slots = groups * CAP
    me = lax.axis_index("shot")
    mine = lax.axis_index("rcv")

    def partner(mask):
        at = me
        for bit in range(bits):
            if mask >> bit & 1:
                own = lax.rem(lax.div(me, 1 << bit), 2)
                at = at + (1 << bit) - own * (2 << bit)
        return at

    partners = [partner(mask) for mask in range(n)]

    def rcv_peer(e):
        return lax.rem(mine + e, groups)

    def cut(h):
        return pl.ds(h * LANES, LANES)

    small = [(code_hbm, code_ref), (blk_hbm, blk_ref), (idx_hbm, idx_ref), (wgt_hbm, wgt_ref),
             (obs_hbm, obs)]
    small = [pltpu.make_async_copy(src, dst, load_sem.at[i]) for i, (src, dst) in enumerate(small)]
    loads = {}
    for h in range(halves):
        for q in range(CUTS):
            some = pl.ds(q * part, part)
            loads[h, q] = pltpu.make_async_copy(
                shot_hbm.at[:, some, cut(h)], shot.at[h, :, some, :],
                load_sem.at[len(small) + h * CUTS + q])
    small[0].start()
    for load in loads.values():
        load.start()
    for load in small[1:]:
        load.start()

    barrier = pltpu.get_barrier_semaphore()
    near = [1 << bit for bit in range(bits)]
    for mask in near:
        pl.semaphore_signal(barrier, inc=1, device_id={"shot": partners[mask]}, device_id_type=MESH)
    for e in range(1, groups):
        pl.semaphore_signal(barrier, inc=1, device_id={"rcv": rcv_peer(e)}, device_id_type=MESH)

    out_rows, depth = n * ROWS, shots * ROWS
    spread_s = (lax.broadcasted_iota(jnp.int32, (shots, depth), 1)
                - ROWS * lax.broadcasted_iota(jnp.int32, (shots, depth), 0))
    spread_s = ((spread_s >= 0) & (spread_s < ROWS)).astype(F32).astype(BF16)

    def widen(j):
        same_row = ((lax.broadcasted_iota(jnp.int32, (out_rows, depth), 0) & (ROWS - 1))
                    == (lax.broadcasted_iota(jnp.int32, (out_rows, depth), 1) & (ROWS - 1)))
        for m in range(n):
            line = code_ref[pl.ds(partners[m] * owned + j, 1), :].astype(F32)
            signs[j, m * ROWS:(m + 1) * ROWS, :] = jnp.broadcast_to(line, (ROWS, shots)).astype(BF16)
        wide = jnp.dot(signs[j], spread_s, preferred_element_type=F32)
        weights[j] = jnp.where(same_row, wide, 0.0).astype(BF16)

    def copy_of(p, slot, count, sem, peer):
        c, row, rows = pieces[p]
        some = pl.ds(row, rows)
        return pltpu.make_async_remote_copy(
            src_ref=send.at[c, pl.ds(slot, count), some], dst_ref=recv.at[c, pl.ds(slot, count), some],
            send_sem=ssem, recv_sem=rsem.at[sem],
            device_id={"shot": partners[peer]}, device_id_type=MESH)

    def copies(p, s):
        kept, peers, _ = table[p][s]
        return [copy_of(p, slot, len(kept), sem_of[p, s], peer) for peer, slot in peers]

    def wait_for(p, s):
        _, peers, (first, count) = table[p][s]
        copy_of(p, first, count, sem_of[p, s], peers[0][0]).wait_recv()

    def copy3(c, e):
        return pltpu.make_async_remote_copy(
            src_ref=send3.at[c, e - 1], dst_ref=recv3.at[c, e], send_sem=s3,
            recv_sem=r3.at[c], device_id={"rcv": rcv_peer(e)}, device_id_type=MESH)

    def copies3(c):
        return pltpu.make_async_remote_copy(
            src_ref=send3.at[c], dst_ref=recv3.at[c, pl.ds(1, groups - 1)], send_sem=s3,
            recv_sem=r3.at[c], device_id={"rcv": rcv_peer(1)}, device_id_type=MESH)

    def copyx(i, e):
        return pltpu.make_async_remote_copy(
            src_ref=sendx.at[i, e - 1], dst_ref=recvx.at[i, e], send_sem=sx,
            recv_sem=rx.at[i], device_id={"rcv": rcv_peer(e)}, device_id_type=MESH)

    def copiesx(i):
        return pltpu.make_async_remote_copy(
            src_ref=sendx.at[i], dst_ref=recvx.at[i, pl.ds(1, groups - 1)], send_sem=sx,
            recv_sem=rx.at[i], device_id={"rcv": rcv_peer(1)}, device_id_type=MESH)

    widened = set()

    def mix(c, row, size, put):
        j, h = c // halves, c % halves
        if j not in widened:
            if not widened:
                small[0].wait()
            widened.add(j)
            widen(j)
        if j == 0:
            loads[h, row // part].wait()

        def tile(g, carry):
            rows = pl.ds(pl.multiple_of(row + g * ROWS, ROWS), ROWS)
            x = shot[h, :, rows, :]
            y = jnp.dot(weights[j], x.reshape(depth, LANES), preferred_element_type=F32)
            put(rows, y.reshape(n, ROWS, LANES))
            return carry

        lax.fori_loop(0, size // ROWS, tile, 0, unroll=min(4, size // ROWS))

    def pick(c, s):
        i, j, h = c - plain, c // halves, c % halves
        if s < CUTS:
            def put(rows, y):
                full[:, rows, :] = y.astype(BF16)

            mix(c, s * part, part, put)
            return
        third = -(-(n + 1) // 3)
        for m in range((s - CUTS) * third, min(n + 1, (s - CUTS + 1) * third)):
            rows = full[m] if m < n else obs[j, :, cut(h)]
            picked = jnp.dot(select[...], rows, preferred_element_type=F32).astype(BF16)
            recvx[i, 0, m] = picked[:CAP]
            for e in range(1, groups):
                sendx[i, e - 1, m] = picked[e * CAP:(e + 1) * CAP]
        if s == CUTS + 2:
            for e in range(1, groups):
                copyx(i, e).start()

    def encode(p, _):
        c, row, size = pieces[p]
        kept, peers, _ = table[p][0]
        if c >= plain:
            i, e, some = c - plain, row // CAP, pl.ds(row, size)
            if row == 0:
                copiesx(i).wait_recv()
            for m in kept:
                acc[c, m, some] = recvx[i, e, m].astype(F32)
            for peer, slot in peers:
                for k, m in enumerate(kept):
                    send[c, slot + k, some] = recvx[i, e, m | peer]
        else:
            def put(rows, y):
                for m in kept:
                    acc[c, m, rows, :] = y[m]
                for peer, slot in peers:
                    for i, m in enumerate(kept):
                        send[c, slot + i, rows, :] = y[m | peer].astype(BF16)

            mix(c, row, size, put)
        if p == 0:
            pl.semaphore_wait(barrier, len(near) + groups - 1)
        for copy in copies(p, 0):
            copy.start()

    def received(p, s, m):
        kept, peers, _ = table[p][s]
        c, row, rows = pieces[p]
        some = pl.ds(row, rows)
        total = acc[c, m, some]
        for _, slot in peers:
            total = total + recv[c, slot + kept.index(m), some].astype(F32)
        return total

    def sum_up(p, s):
        wait_for(p, s)
        kept, peers, _ = table[p][s + 1]
        c, row, rows = pieces[p]
        some = pl.ds(row, rows)
        for (peer, slot), copy in zip(peers, copies(p, s + 1)):
            for i, m in enumerate(kept):
                send[c, slot + i, some] = received(p, s, m | peer).astype(BF16)
            copy.start()
        for m in kept:
            acc[c, m, some] = received(p, s, m)

    def finish(c, _):
        j, h = c // halves, c % halves
        for p in members[c]:
            _, row, rows = pieces[p]
            some = pl.ds(row, rows)
            wait_for(p, len(table[p]) - 1)
            seen = obs[j, some, cut(h)] if c < plain else recvx[c - plain, row // CAP, n]
            residual = received(p, len(table[p]) - 1, 0) - seen.astype(F32)
            left[c, some] = residual.astype(BF16)
        if c >= plain:
            out[j, :, cut(h)] = jnp.dot(slotm[...], left[c], preferred_element_type=F32)
            return
        picked = jnp.dot(select[...], left[c], preferred_element_type=F32).astype(BF16)
        for e in range(1, groups):
            send3[c, e - 1] = picked[e * CAP:(e + 1) * CAP]
            copy3(c, e).start()
        recv3[c, 0] = picked[:CAP]

    def inject(c, _):
        copies3(c).wait_recv()
        arrived = recv3[c].reshape(slots, LANES)
        j, h = c // halves, c % halves
        out[j, :, cut(h)] = jnp.dot(slotm[...], arrived, preferred_element_type=F32)

    def prepare():
        before = (lax.broadcasted_iota(jnp.int32, (rcv, rcv), 0)
                  < lax.broadcasted_iota(jnp.int32, (rcv, rcv), 1)).astype(F32).astype(BF16)
        slot_at = lax.broadcasted_iota(jnp.int32, (slots, rcv), 0)
        point_at = lax.broadcasted_iota(jnp.int32, (GRID, rcv), 0)
        block_at = lax.broadcasted_iota(jnp.int32, (max(16, groups), rcv), 0)

        def rank_of(ids):
            hot = (block_at == ids).astype(F32)
            count = jnp.dot(hot.astype(BF16), before, preferred_element_type=F32)
            return jnp.sum(hot * count, axis=0, keepdims=True).astype(jnp.int32)

        total = jnp.zeros((GRID, slots), F32)
        for e in range(groups):
            source = lax.rem(mine - e + groups, groups)
            at = pl.ds(pl.multiple_of(source * rcv, rcv), rcv)
            ids = blk_ref[:, at]
            rank = rank_of(ids)
            if e == 0:
                ahead = ids - mine
                ahead = jnp.where(ahead < 0, ahead + groups, ahead)
                select[...] = (slot_at == ahead * CAP + rank).astype(F32).astype(BF16)
            spread = jnp.zeros((GRID, rcv), F32)
            for w in range(idx_ref.shape[0]):
                spread = spread + jnp.where(
                    point_at == idx_ref[pl.ds(w, 1), at], wgt_ref[pl.ds(w, 1), at], 0.0)
            key = jnp.where(ids == mine, e * CAP + rank, -1)
            pick = (slot_at == key).astype(F32).astype(BF16)
            total = total + lax.dot_general(
                spread.astype(BF16), pick, (((1,), (1,)), ((), ())), preferred_element_type=F32)
        slotm[...] = total.astype(BF16)

    act = {"pick": pick, "encode": encode, "sum": sum_up, "finish": finish, "inject": inject}
    prepared = False
    for _, _, item, what, s in tasks:
        if what != "encode" and not prepared:
            for load in small[1:]:
                load.wait()
            prepare()
            prepared = True
        act[what](item, s)
    pltpu.make_async_remote_copy(
        src_ref=send, dst_ref=recv, send_sem=ssem, recv_sem=rsem.at[0],
        device_id={"shot": partners[1]}, device_id_type=MESH).wait_send()
    pltpu.make_async_remote_copy(
        src_ref=send3, dst_ref=send3, send_sem=s3, recv_sem=r3.at[0],
        device_id={"rcv": rcv_peer(1)}, device_id_type=MESH).wait_send()
    if early:
        pltpu.make_async_remote_copy(
            src_ref=sendx, dst_ref=sendx, send_sem=sx, recv_sem=rx.at[0],
            device_id={"rcv": rcv_peer(1)}, device_id_type=MESH).wait_send()


def on_device(n_shot, n_rcv, shot_data, code, observed, block_of, stencil_index, stencil_weight):
    shots, rcv, samples = shot_data.shape
    owned = observed.shape[0]
    halves = samples // LANES
    chunks = owned * halves
    pieces = cut_up(chunks, rcv)
    slots = n_rcv * CAP
    part = rcv // CUTS
    table = plan(len(pieces), n_shot.bit_length() - 1)
    members = members_of(pieces)
    early = EARLY if slots == rcv and part == CAP and SPLIT == 0 else 0
    tasks = schedule(table, members, early)
    kinds = max(early, 1)
    plain = chunks - early
    sem_of, sems = share_out(table, tasks, members)
    hbm = pl.BlockSpec(memory_space=pltpu.HBM)
    vmem = pltpu.VMEM
    dma = pltpu.SemaphoreType.DMA
    rows = (block_of.T, stencil_index.T, stencil_weight.T)
    return pl.pallas_call(
        functools.partial(kernel, (n_shot, n_rcv, owned, halves, early), pieces, table, tasks, sem_of),
        out_shape=pltpu.VMEM((owned, GRID, samples), F32),
        in_specs=[hbm] * 6,
        out_specs=pl.BlockSpec(memory_space=vmem),
        scratch_shapes=[
            vmem((halves, shots, rcv, LANES), BF16),
            vmem(code.shape, code.dtype),
            vmem((owned, rcv, samples), BF16),
            *[vmem(row.shape, row.dtype) for row in rows],
            vmem((owned, n_shot * ROWS, shots), BF16),
            vmem((owned, n_shot * ROWS, shots * ROWS), BF16),
            vmem((chunks, n_shot, rcv, LANES), F32),
            vmem((chunks, n_shot - 1, rcv, LANES), BF16),
            vmem((chunks, n_shot - 1, rcv, LANES), BF16),
            vmem((plain, n_rcv - 1, CAP, LANES), BF16),
            vmem((plain, n_rcv, CAP, LANES), BF16),
            vmem((chunks, rcv, LANES), BF16),
            vmem((n_shot, rcv, LANES), BF16),
            vmem((kinds, n_rcv - 1, n_shot + 1, CAP, LANES), BF16),
            vmem((kinds, n_rcv, n_shot + 1, CAP, LANES), BF16),
            vmem((slots, rcv), BF16),
            vmem((GRID, slots), BF16),
            dma((5 + halves * CUTS,)),
            dma,
            dma((sems,)),
            dma,
            dma((plain,)),
            dma,
            dma((kinds,)),
        ],
        compiler_params=pltpu.CompilerParams(
            collective_id=0, has_side_effects=True, vmem_limit_bytes=40 * 2**20),
    )(*[pltpu.with_memory_space_constraint(x, pltpu.HBM)
        for x in (shot_data, code, observed, *rows)])


def solution(mesh):
    placed = (P("shot", "rcv", None), P(None, "shot"), P("shot", "rcv", None), P(), P(), P())
    body = functools.partial(on_device, mesh.shape["shot"], mesh.shape["rcv"])
    return jax.shard_map(
        body, mesh=mesh, in_specs=placed, out_specs=P("shot", "rcv", None), check_vma=False
    )
```
